32 devices in a mesh: dp: 8 (over z, y), vp: 4 (over x, core).
Axes of the slice: x: 2, y: 2, z: 4, core: 2. Of those that a mesh axis runs over, the one named last changes fastest.
Arguments:
- hidden: bfloat16 [8, 2048, 768], P('dp', 'vp')
- targets: int32 [8, 2048], P('dp', 'vp')
- loss_mask: int32 [8, 2048], P('dp', 'vp')
- norm_scale: float32 [768], replicated
- w_head: bfloat16 [768, 65536], P(None, 'vp')
Outputs:
- output 1: float32 [], replicated
- output 2: bfloat16 [8, 2048, 768], P('dp', 'vp')
- output 3: float32 [768, 65536], P(None, 'vp')
- output 4: float32 [768], replicated
All inputs are finite; a program needn't handle non-finite values.
Results may differ from the reference program's by a relative error of at most 0.001.
Values sent between devices are 32-bit elements.
A program may use at most 1 GiB of HBM per device.

```python
import jax
import jax.numpy as jnp
import math
from jax import lax

MODEL_DIM = 768
VOCAB_SIZE = 65536
DP_SIZE = 8
VP_SIZE = 4
BATCH_DEV = 1
TOK_DEV = 512

EPS = 1e-5
VOCAB_PAD = ((VOCAB_SIZE + 128 * VP_SIZE - 1) // (128 * VP_SIZE)) * 128 * VP_SIZE
BATCH = DP_SIZE * BATCH_DEV
SEQ_LEN = VP_SIZE * TOK_DEV


def setup_inputs(seed: int = 0) -> dict:
    key = jax.random.key(seed)
    k_hid, k_tgt, k_pct, k_msk, k_scale, k_w, k_col, k_blk = jax.random.split(key, 8)
    hidden = jax.random.normal(k_hid, (BATCH, SEQ_LEN, MODEL_DIM), jnp.float32).astype(jnp.bfloat16)
    targets = jax.random.randint(k_tgt, (BATCH, SEQ_LEN), 0, VOCAB_SIZE, jnp.int32)
    targets = targets.at[0, 0].set(0).at[BATCH - 1, SEQ_LEN - 1].set(VOCAB_SIZE - 1)
    keep_pct = jnp.repeat(jax.random.randint(k_pct, (DP_SIZE,), 10, 96, jnp.int32), BATCH_DEV)
    draws = jax.random.randint(k_msk, (BATCH, SEQ_LEN), 0, 100, jnp.int32)
    loss_mask = (draws < keep_pct[:, None]).astype(jnp.int32)
    loss_mask = loss_mask.at[0, 0].set(1).at[0, 1].set(0)
    norm_scale = jax.random.uniform(k_scale, (MODEL_DIM,), jnp.float32, 0.5, 1.5)
    col_scale = jnp.exp(0.35 * jax.random.normal(k_col, (VOCAB_PAD,), jnp.float32))
    blk_scale = jnp.repeat(jnp.exp(0.3 * jax.random.normal(k_blk, (VOCAB_PAD // 128,), jnp.float32)), 128)
    fan_scale = 1.0 / math.sqrt(MODEL_DIM)
    w_f32 = jax.random.normal(k_w, (MODEL_DIM, VOCAB_PAD), jnp.float32) * fan_scale
    w_head = (w_f32 * (col_scale * blk_scale)).astype(jnp.bfloat16)
    return {'hidden': hidden, 'targets': targets, 'loss_mask': loss_mask, 'norm_scale': norm_scale, 'w_head': w_head}


def rms_norm(x_rows, norm_scale):
    inv_rms = lax.rsqrt(jnp.mean(x_rows * x_rows, axis=-1, keepdims=True) + EPS)
    return x_rows * inv_rms * norm_scale


def reference(hidden, targets, loss_mask, norm_scale, w_head):
    num_blocks = BATCH * SEQ_LEN // TOK_DEV
    mask_f = loss_mask.astype(jnp.float32)
    tok_weight = (mask_f / jnp.sum(mask_f)).reshape(num_blocks, TOK_DEV)
    x_blocks = hidden.reshape(num_blocks, TOK_DEV, MODEL_DIM)
    tgt_blocks = targets.reshape(num_blocks, TOK_DEV)
    col_ids = lax.broadcasted_iota(jnp.int32, (1, VOCAB_PAD), 1)

    def block_step(carried, block_in):
        loss_acc, dscale_acc, dw_acc = carried
        x_blk, tgt_blk, wt_blk = block_in
        normed_f, norm_vjp = jax.vjp(rms_norm, x_blk.astype(jnp.float32), norm_scale)
        normed = normed_f.astype(jnp.bfloat16)
        logits = jnp.dot(normed, w_head, preferred_element_type=jnp.float32)
        row_max = jnp.max(logits, axis=-1, keepdims=True)
        exp_logits = jnp.exp(logits - row_max)
        row_sum = jnp.sum(exp_logits, axis=-1, keepdims=True)
        log_norm = row_max[:, 0] + jnp.log(row_sum[:, 0])
        is_target = col_ids == tgt_blk[:, None]
        tgt_logit = jnp.sum(jnp.where(is_target, logits, 0.0), axis=-1)
        loss_acc = loss_acc + jnp.sum(wt_blk * (log_norm - tgt_logit))
        d_logits = ((exp_logits / row_sum - is_target.astype(jnp.float32)) * wt_blk[:, None]).astype(jnp.bfloat16)
        d_normed = jnp.dot(d_logits, w_head.T, preferred_element_type=jnp.float32)
        d_x, d_scale = norm_vjp(d_normed)
        dw_acc = dw_acc + jnp.dot(normed.T, d_logits, preferred_element_type=jnp.float32)
        return (loss_acc, dscale_acc + d_scale, dw_acc), d_x.astype(jnp.bfloat16)

    init_carry = (jnp.zeros((), jnp.float32), jnp.zeros((MODEL_DIM,), jnp.float32), jnp.zeros((MODEL_DIM, VOCAB_PAD), jnp.float32))
    (total_loss, d_scale, d_w), d_x = lax.scan(block_step, init_carry, (x_blocks, tgt_blocks, tok_weight))
    return total_loss, d_x.reshape(BATCH, SEQ_LEN, MODEL_DIM), d_w, d_scale
```

```python
import functools

import jax
import jax.numpy as jnp
from jax import lax
from jax.experimental import pallas as pl
from jax.experimental.pallas import tpu as pltpu
from jax.sharding import PartitionSpec as P


EPS = 1e-5
BLK = 512
DIM = 768
ALIGN = 16
FWD_COLS = 1024
DN_COLS = 512
DW_COLS = 512
DW_TOK = 1024
SUB = 256
DROPPED = 1e30


f32, bf16, i32 = jnp.float32, jnp.bfloat16, jnp.int32


def place_tokens(offs_ref, count, dst, get):
    for b in range(count):
        off = pl.multiple_of(offs_ref[b], ALIGN)
        dst[pl.ds(off, BLK), :] = get(b)


def aux_columns(aux):
    pad = jnp.zeros((120, BLK), f32)
    return jnp.concatenate([aux, pad], axis=0).T


def fwd_kernel(offs_ref, nt_ref, xh_ref, g_ref, w_ref, n_ref, st_ref, m_ref, s_ref):
    j = pl.program_id(0)

    @pl.when(j == 0)
    def _():
        n_ref[...] = jnp.zeros_like(n_ref)
        m_ref[...] = jnp.full_like(m_ref, -DROPPED)
        s_ref[...] = jnp.zeros_like(s_ref)
        place_tokens(offs_ref, 4, n_ref, lambda b: (xh_ref[pl.ds(b * BLK, BLK), :] * g_ref[...]).astype(bf16))

    def tile(i, carry):
        for u in range(2):
            rows = pl.ds(pl.multiple_of(i * 256, 256) + u * 128, 128)
            z = jnp.dot(n_ref[rows, :], w_ref[...], preferred_element_type=f32)
            parts = [z[:, k * 128 : (k + 1) * 128] for k in range(FWD_COLS // 128)]
            m_old = m_ref[rows, :]
            m_new = functools.reduce(jnp.maximum, parts, m_old)
            total = s_ref[rows, :] * jnp.exp(m_old - m_new)
            for part in parts:
                total += jnp.exp(part - m_new)
            m_ref[rows, :] = m_new
            s_ref[rows, :] = total
        return carry

    lax.fori_loop(0, nt_ref[0], tile, 0)

    @pl.when(j == pl.num_programs(0) - 1)
    def _():
        for b in range(4):
            rows = pl.ds(pl.multiple_of(offs_ref[b], ALIGN), BLK)
            m_lane = m_ref[rows, :]
            m = jnp.max(m_lane, axis=1, keepdims=True)
            s = jnp.sum(s_ref[rows, :] * jnp.exp(m_lane - m), axis=1, keepdims=True)
            st_ref[b, 0:1, :] = jnp.broadcast_to(m, (BLK, 128)).T[0:1, :]
            st_ref[b, 1:2, :] = jnp.broadcast_to(s, (BLK, 128)).T[0:1, :]


def forward_stats(offs, ntiles, xh_row, g, w):
    vocab = w.shape[1]
    steps = vocab // FWD_COLS
    return pl.pallas_call(
        fwd_kernel,
        grid_spec=pltpu.PrefetchScalarGridSpec(
            num_scalar_prefetch=2,
            grid=(steps,),
            in_specs=[
                pl.BlockSpec((4 * BLK, DIM), lambda j, *_: (0, 0)),
                pl.BlockSpec((1, DIM), lambda j, *_: (0, 0)),
                pl.BlockSpec((DIM, FWD_COLS), lambda j, *_: (0, j)),
            ],
            out_specs=[
                pl.BlockSpec((4 * BLK, DIM), lambda j, *_: (0, 0)),
                pl.BlockSpec((4, 2, BLK), lambda j, *_: (0, 0, 0)),
            ],
            scratch_shapes=[pltpu.VMEM((4 * BLK, 128), f32), pltpu.VMEM((4 * BLK, 128), f32)],
        ),
        out_shape=[
            jax.ShapeDtypeStruct((4 * BLK, DIM), bf16),
            jax.ShapeDtypeStruct((4, 2, BLK), f32),
        ],
        compiler_params=pltpu.CompilerParams(dimension_semantics=("arbitrary",)),
        cost_estimate=pl.CostEstimate(
            flops=2 * 4 * BLK * DIM * vocab, bytes_accessed=2 * DIM * vocab + 10 * BLK * DIM * 4, transcendentals=4 * BLK * vocab
        ),
        name="fwd_stats",
    )(offs, ntiles, xh_row, g, w)


def grad_logits(z, aux, col0):
    target = aux[:, 2:3].astype(i32) - col0
    hot = lax.broadcasted_iota(i32, z.shape, 1) == target
    p = jnp.exp(z - aux[:, 0:1])
    dz = (jnp.where(hot, p - 1.0, p) * aux[:, 1:2]).astype(bf16)
    return dz, hot


def dn_kernel(offs_ref, kept_ref, nt_ref, col_ref, n_ref, aux_ref, w_ref, dn_ref, tl_ref, acc_ref, auxc_ref):
    j = pl.program_id(0)

    @pl.when(j == 0)
    def _():
        acc_ref[...] = jnp.zeros_like(acc_ref)
        auxc_ref[...] = jnp.zeros_like(auxc_ref)
        tl_ref[...] = jnp.zeros_like(tl_ref)
        place_tokens(offs_ref, 4, auxc_ref, lambda b: aux_columns(aux_ref[b]))

    col0 = col_ref[0] + j * DN_COLS

    def tile(i, carry):
        rows = pl.ds(pl.multiple_of(i * 256, 256), 256)
        aux = auxc_ref[rows, :]
        z = jnp.dot(n_ref[rows, :], w_ref[...], preferred_element_type=f32)
        dz, hot = grad_logits(z, aux, col0)
        picked = jnp.where(hot, z, 0.0)
        picked = functools.reduce(jnp.add, [picked[:, k * 128 : (k + 1) * 128] for k in range(DN_COLS // 128)])
        tl_ref[...] += jnp.sum((picked * aux[:, 1:2]).reshape(32, 8, 128), axis=0)
        acc_ref[rows, :] += lax.dot_general(dz, w_ref[...], (((1,), (1,)), ((), ())), preferred_element_type=f32)
        return carry

    lax.fori_loop(0, nt_ref[0], tile, 0)

    @pl.when(j == pl.num_programs(0) - 1)
    def _():
        for b in range(4):
            got = acc_ref[pl.ds(pl.multiple_of(offs_ref[b], ALIGN), BLK), :]
            live = lax.broadcasted_iota(i32, (BLK, 1), 0) < kept_ref[b]
            dn_ref[pl.ds(b * BLK, BLK), :] = jnp.where(live, got, 0.0)


def backward_dn(offs, kept, ntiles, col0, n_row, aux_row, w):
    vocab = w.shape[1]
    return pl.pallas_call(
        dn_kernel,
        grid_spec=pltpu.PrefetchScalarGridSpec(
            num_scalar_prefetch=4,
            grid=(vocab // DN_COLS,),
            in_specs=[
                pl.BlockSpec((4 * BLK, DIM), lambda j, *_: (0, 0)),
                pl.BlockSpec((4, 8, BLK), lambda j, *_: (0, 0, 0)),
                pl.BlockSpec((DIM, DN_COLS), lambda j, *_: (0, j)),
            ],
            out_specs=[
                pl.BlockSpec((4 * BLK, DIM), lambda j, *_: (0, 0)),
                pl.BlockSpec((8, 128), lambda j, *_: (0, 0)),
            ],
            scratch_shapes=[pltpu.VMEM((4 * BLK, DIM), f32), pltpu.VMEM((4 * BLK, 128), f32)],
        ),
        out_shape=[
            jax.ShapeDtypeStruct((4 * BLK, DIM), f32),
            jax.ShapeDtypeStruct((8, 128), f32),
        ],
        compiler_params=pltpu.CompilerParams(dimension_semantics=("arbitrary",)),
        cost_estimate=pl.CostEstimate(
            flops=4 * 4 * BLK * DIM * vocab, bytes_accessed=2 * DIM * vocab + 6 * BLK * DIM * 4, transcendentals=4 * BLK * vocab
        ),
        name="backward_dn",
    )(offs, kept, ntiles, col0, n_row, aux_row, w)


def gather_kernel(offs_ref, xh_ref, g_ref, aux_ref, n_hbm, aux_hbm, n_ref, auxc_ref, sems):
    b = pl.program_id(0)

    @pl.when(b == 0)
    def _():
        auxc_ref[...] = jnp.zeros_like(auxc_ref)

        def clear(i, carry):
            n_ref[pl.ds(pl.multiple_of(i * BLK, BLK), BLK), :] = jnp.zeros((BLK, DIM), bf16)
            return carry

        lax.fori_loop(0, n_ref.shape[0] // BLK, clear, 0)

    off = pl.multiple_of(offs_ref[b], ALIGN)
    n_ref[pl.ds(off, BLK), :] = (xh_ref[...] * g_ref[...]).astype(bf16)
    auxc_ref[pl.ds(off, BLK), :] = aux_columns(aux_ref[0])

    @pl.when(b == pl.num_programs(0) - 1)
    def _():
        copies = [pltpu.make_async_copy(n_ref, n_hbm, sems.at[0]), pltpu.make_async_copy(auxc_ref, aux_hbm, sems.at[1])]
        for copy in copies:
            copy.start()
        for copy in copies:
            copy.wait()


def gather_tokens(offs, xh_all, g, aux_all):
    blocks = aux_all.shape[0]
    tokens = blocks * BLK
    return pl.pallas_call(
        gather_kernel,
        grid_spec=pltpu.PrefetchScalarGridSpec(
            num_scalar_prefetch=1,
            grid=(blocks,),
            in_specs=[
                pl.BlockSpec((BLK, DIM), lambda b, *_: (b, 0)),
                pl.BlockSpec((1, DIM), lambda b, *_: (0, 0)),
                pl.BlockSpec((1, 8, BLK), lambda b, *_: (b, 0, 0)),
            ],
            out_specs=[pl.BlockSpec(memory_space=pl.ANY), pl.BlockSpec(memory_space=pl.ANY)],
            scratch_shapes=[
                pltpu.VMEM((tokens, DIM), bf16),
                pltpu.VMEM((tokens, 128), f32),
                pltpu.SemaphoreType.DMA((2,)),
            ],
        ),
        out_shape=[
            jax.ShapeDtypeStruct((tokens, DIM), bf16),
            jax.ShapeDtypeStruct((tokens, 128), f32),
        ],
        compiler_params=pltpu.CompilerParams(dimension_semantics=("arbitrary",), vmem_limit_bytes=56 << 20),
        cost_estimate=pl.CostEstimate(flops=2 * tokens * DIM, bytes_accessed=6 * tokens * DIM, transcendentals=0),
        name="gather_tokens",
    )(offs, xh_all, g, aux_all)


def dw_kernel(place_ref, nt_ref, n_hbm, aux_hbm, w_ref, *rest):
    out_ref, all_ref, nbuf, abuf, sems = rest[-5:]
    steps = nt_ref[0]

    def fetch(i, slot):
        rows = pl.ds(pl.multiple_of(i * DW_TOK, DW_TOK), DW_TOK)
        return (
            pltpu.make_async_copy(n_hbm.at[rows, :], nbuf.at[slot], sems.at[slot, 0]),
            pltpu.make_async_copy(aux_hbm.at[rows, :], abuf.at[slot], sems.at[slot, 1]),
        )

    for copy in fetch(0, 0):
        copy.start()
    out_ref[...] = jnp.zeros_like(out_ref)

    def tile(i, carry):
        slot = lax.rem(i, 2)

        @pl.when(i + 1 < steps)
        def _():
            for copy in fetch(i + 1, 1 - slot):
                copy.start()

        for copy in fetch(i, slot):
            copy.wait()
        for u in range(DW_TOK // SUB):
            rows = pl.ds(u * SUB, SUB)
            n = nbuf[slot, rows, :]
            z = jnp.dot(n, w_ref[...], preferred_element_type=f32)
            dz, _ = grad_logits(z, abuf[slot, rows, :], place_ref[1])
            out_ref[...] += lax.dot_general(n, dz, (((0,), (0,)), ((), ())), preferred_element_type=f32)
        return carry

    lax.fori_loop(0, steps, tile, 0)
    all_ref[...] = out_ref[...]


def weight_grad(place, ntiles, n_all, aux_all, w, whole):
    tokens, vocab = n_all.shape[0], w.shape[1]
    column = pl.BlockSpec((DIM, DW_COLS), lambda i, place, nt: (0, place[0]))
    anywhere = pl.BlockSpec(memory_space=pl.ANY)
    held = [] if whole is None else [whole]
    return pl.pallas_call(
        dw_kernel,
        grid_spec=pltpu.PrefetchScalarGridSpec(
            num_scalar_prefetch=2,
            grid=(1,),
            in_specs=[anywhere, anywhere, column] + [anywhere] * len(held),
            out_specs=[pl.BlockSpec((DIM, DW_COLS), lambda i, *_: (0, 0)), column],
            scratch_shapes=[
                pltpu.VMEM((2, DW_TOK, DIM), bf16),
                pltpu.VMEM((2, DW_TOK, 128), f32),
                pltpu.SemaphoreType.DMA((2, 2)),
            ],
        ),
        out_shape=[
            jax.ShapeDtypeStruct((DIM, DW_COLS), f32),
            jax.ShapeDtypeStruct((DIM, vocab), f32),
        ],
        input_output_aliases={5: 1} if held else {},
        compiler_params=pltpu.CompilerParams(dimension_semantics=("arbitrary",)),
        cost_estimate=pl.CostEstimate(
            flops=2 * tokens * DIM * DW_COLS, bytes_accessed=tokens * DIM + 8 * DIM * DW_COLS, transcendentals=tokens * DW_COLS // 2
        ),
        name="weight_grad",
    )(place, ntiles.reshape(1), n_all, aux_all, w, *held)


def solution(mesh):
    dp_count, vp_count = mesh.shape["dp"], mesh.shape["vp"]

    def local_step(hidden, targets, loss_mask, norm_scale, w_head):
        vocab = w_head.shape[1]
        dp, vp = lax.axis_index("dp"), lax.axis_index("vp")
        g = norm_scale.reshape(1, DIM)

        mask = loss_mask[0]
        idx = lax.iota(i32, BLK)
        before = jnp.sum(jnp.where(idx[None, :] < idx[:, None], mask[None, :], 0), axis=1)
        kept = jnp.sum(mask)
        pos = jnp.where(mask == 1, before, kept + idx - before)
        perm = pos[None, :] == idx[:, None]
        x_sorted = jnp.dot(perm.astype(bf16), hidden[0], preferred_element_type=f32)
        t_sorted = jnp.sum(jnp.where(perm, targets[0][None, :], 0), axis=1)
        inv_rms = lax.rsqrt(jnp.mean(x_sorted * x_sorted, axis=-1, keepdims=True) + EPS)
        x_hat = x_sorted * inv_rms

        xh_row = lax.all_gather(x_hat, "vp", axis=0, tiled=True)
        info = jnp.concatenate([t_sorted, jnp.full((BLK,), kept, i32)]).reshape(1, 2 * BLK)
        info = lax.all_gather(info, ("dp", "vp"), axis=0, tiled=True)
        xh_all = lax.all_gather(x_hat, ("dp", "vp"), axis=0, tiled=True)

        t_all, kept_all = info[:, :BLK], info[:, BLK]
        span = (kept_all + ALIGN - 1) // ALIGN * ALIGN
        offs_all = jnp.cumsum(span) - span
        total = jnp.sum(span)
        weight = 1.0 / jnp.sum(kept_all).astype(f32)
        kept_row = lax.dynamic_slice(kept_all, (dp * vp_count,), (vp_count,))
        offs_row = lax.dynamic_slice(offs_all, (dp * vp_count,), (vp_count,))
        span_row = lax.dynamic_slice(span, (dp * vp_count,), (vp_count,))
        offs_row = offs_row - offs_row[0]
        nt_row = ((jnp.sum(span_row) + 255) // 256).reshape(1)
        nt_all = jnp.maximum((total + DW_TOK - 1) // DW_TOK, 1)

        n_row, stats = forward_stats(offs_row, nt_row, xh_row, g, w_head)
        stats = lax.all_gather(stats, "vp", axis=0)
        row_max = jnp.max(stats[:, :, 0], axis=0)
        row_sum = jnp.sum(stats[:, :, 1] * jnp.exp(stats[:, :, 0] - row_max), axis=0)
        lse_row = row_max + jnp.log(row_sum)
        live_row = idx[None, :] < kept_row[:, None]
        lse_row = jnp.where(live_row, lse_row, DROPPED)
        lse_all = lax.all_gather(lse_row, "dp", axis=0, tiled=True)
        live_all = idx[None, :] < kept_all[:, None]
        w_all = jnp.where(live_all, weight, 0.0)
        zeros = jnp.zeros_like(w_all)
        aux_all = jnp.stack([lse_all, w_all, t_all.astype(f32)] + [zeros] * 5, axis=1)
        aux_row = lax.dynamic_slice(aux_all, (dp * vp_count, 0, 0), (vp_count, 8, BLK))

        dn_part, t_part = backward_dn(offs_row, kept_row, nt_row, (vp * vocab).reshape(1), n_row, aux_row, w_head)
        d_normed = lax.psum_scatter(dn_part, "vp", scatter_dimension=0, tiled=True)

        n_all, auxc_all = gather_tokens(offs_all, xh_all, g, aux_all)
        half, quarter = vocab // 2, vocab // 4
        y_pos, z_pos = dp % 2, (dp // 2) % 2
        y_pairs = [(d, d ^ 1) for d in range(dp_count)]
        z_pairs = [(d, d ^ 2) for d in range(dp_count)]
        whole, moved = None, []
        for c in range(quarter // DW_COLS):
            for base, where, pairs in ((0, y_pos, y_pairs), (half, z_pos, z_pairs)):
                col = base + where * quarter + c * DW_COLS
                place = jnp.stack([col // DW_COLS, vp * vocab + col]).astype(i32)
                chunk, whole = weight_grad(place, nt_all, n_all, auxc_all, w_head, whole)
                other = base + (1 - where) * quarter + c * DW_COLS
                moved.append((other, lax.ppermute(chunk, "dp", pairs)))
        for other, chunk in moved:
            whole = lax.dynamic_update_slice(whole, chunk, (0, other))

        d_scale = jnp.sum(d_normed * x_hat, axis=0)
        e = d_normed * norm_scale
        d_x = inv_rms * (e - x_hat * jnp.mean(e * x_hat, axis=-1, keepdims=True))
        back = perm.astype(bf16).T
        d_x = jnp.dot(back, d_x.astype(bf16), preferred_element_type=f32).astype(bf16)

        own = jnp.where(idx < kept, lax.dynamic_slice(lse_row, (vp, 0), (1, BLK))[0], 0.0)
        loss_part = weight * jnp.sum(own) - jnp.sum(t_part)
        parts = jnp.concatenate([d_scale, jnp.full((128,), loss_part, f32)]).reshape(1, DIM + 128)
        parts = jnp.sum(lax.all_gather(parts, ("dp", "vp"), axis=0, tiled=True), axis=0)
        return parts[DIM], d_x[None], whole, parts[:DIM]

    return jax.shard_map(
        local_step,
        mesh=mesh,
        in_specs=(P("dp", "vp", None), P("dp", "vp"), P("dp", "vp"), P(None), P(None, "vp")),
        out_specs=(P(), P("dp", "vp", None), P(None, "vp"), P(None)),
        check_vma=False,
    )
```

```python
import functools

import jax
import jax.numpy as jnp
from jax import lax
from jax.experimental import pallas as pl
from jax.experimental.pallas import tpu as pltpu
from jax.sharding import PartitionSpec as P


EPS = 1e-5
BLK = 512
DIM = 768
ALIGN = 16
FWD_COLS = 1024
DN_COLS = 2048
DW_COLS = 512
DW_STEPS = 2
DW_TOK = 1024
SUB = 256
LAG = 3
DROPPED = 1e30


f32, bf16, i32 = jnp.float32, jnp.bfloat16, jnp.int32


def tiny_gather_kernel(dp_count, vp_count, x_ref, out_ref, send_sems, recv_sems):
    count = dp_count * vp_count
    me = lax.axis_index("dp") * vp_count + lax.axis_index("vp")
    barrier = pltpu.get_barrier_semaphore()

    def peer(k):
        other = lax.rem(me + k, count)
        return (other // vp_count, lax.rem(other, vp_count))

    for k in range(1, count):
        pl.semaphore_signal(barrier, inc=1, device_id=peer(k), device_id_type=pl.DeviceIdType.MESH)
    pl.semaphore_wait(barrier, count - 1)
    copies = [
        pltpu.make_async_remote_copy(
            src_ref=x_ref,
            dst_ref=out_ref.at[me],
            send_sem=send_sems.at[k - 1],
            recv_sem=recv_sems.at[k - 1],
            device_id=peer(k),
            device_id_type=pl.DeviceIdType.MESH,
        )
        for k in range(1, count)
    ]
    for copy in copies:
        copy.start()
    out_ref[me] = x_ref[...]
    for copy in copies:
        copy.wait()


def tiny_gather(x, mesh_shape, collective_id):
    dp_count, vp_count = mesh_shape
    count = dp_count * vp_count
    return pl.pallas_call(
        functools.partial(tiny_gather_kernel, dp_count, vp_count),
        out_shape=jax.ShapeDtypeStruct((count, 8, 128), f32),
        in_specs=[pl.BlockSpec(memory_space=pltpu.VMEM)],
        out_specs=pl.BlockSpec(memory_space=pltpu.VMEM),
        scratch_shapes=[pltpu.SemaphoreType.DMA((count - 1,)), pltpu.SemaphoreType.DMA((count - 1,))],
        compiler_params=pltpu.CompilerParams(collective_id=collective_id, has_side_effects=True),
        name="tiny_gather",
    )(x)


def place_masked(dst, off, span, new):
    rows = pl.ds(pl.multiple_of(off, ALIGN), BLK)
    live = lax.broadcasted_iota(i32, (BLK, 1), 0) < span
    dst[rows, :] = jnp.where(live, new, dst[rows, :].astype(f32)).astype(dst.dtype)


def aux_columns(aux):
    pad = jnp.zeros((120, BLK), f32)
    return jnp.concatenate([aux, pad], axis=0).T


def fwd_kernel(offs_ref, span_ref, nt_ref, xa, xb, xc, xd, g_ref, w_ref, n_ref, st_ref, m_ref, s_ref, z_ref):
    j = pl.program_id(0)
    steps = nt_ref[0]

    @pl.when(j == 0)
    def _():
        n_ref[...] = jnp.zeros_like(n_ref)
        m_ref[...] = jnp.full_like(m_ref, -DROPPED)
        s_ref[...] = jnp.zeros_like(s_ref)
        for k, x_ref in enumerate((xa, xb, xc, xd)):
            place_masked(n_ref, offs_ref[k], span_ref[k], x_ref[...] * g_ref[...])

    def absorb(rows, z):
        parts = [z[:, k * 128 : (k + 1) * 128] for k in range(FWD_COLS // 128)]
        m_old = m_ref[rows, :]
        m_new = functools.reduce(jnp.maximum, parts, m_old)
        total = s_ref[rows, :] * jnp.exp(m_old - m_new)
        for part in parts:
            total += jnp.exp(part - m_new)
        m_ref[rows, :] = m_new
        s_ref[rows, :] = total

    def rows_of(i, u):
        return pl.ds(pl.multiple_of(i * BLK, BLK) + u * SUB, SUB)

    z_ref[...] = jnp.full_like(z_ref, -DROPPED)

    def tile(i, carry):
        z = jnp.dot(n_ref[rows_of(i, 0), :], w_ref[...], preferred_element_type=f32)
        absorb(rows_of(jnp.maximum(i - 1, 0), 1), z_ref[...])
        z_ref[...] = jnp.dot(n_ref[rows_of(i, 1), :], w_ref[...], preferred_element_type=f32)
        absorb(rows_of(i, 0), z)
        return carry

    lax.fori_loop(0, steps, tile, 0)
    absorb(rows_of(jnp.maximum(steps - 1, 0), 1), z_ref[...])

    @pl.when(j == pl.num_programs(0) - 1)
    def _():
        for k in range(4):
            rows = pl.ds(pl.multiple_of(offs_ref[k], ALIGN), BLK)
            m_lane = m_ref[rows, :]
            m = jnp.max(m_lane, axis=1, keepdims=True)
            s = jnp.sum(s_ref[rows, :] * jnp.exp(m_lane - m), axis=1, keepdims=True)
            st_ref[k, 0:1, :] = jnp.broadcast_to(m, (BLK, 128)).T[0:1, :]
            st_ref[k, 1:2, :] = jnp.broadcast_to(s, (BLK, 128)).T[0:1, :]


def forward_stats(offs, span, ntiles, blocks, g, w):
    vocab = w.shape[1]
    return pl.pallas_call(
        fwd_kernel,
        grid_spec=pltpu.PrefetchScalarGridSpec(
            num_scalar_prefetch=3,
            grid=(vocab // FWD_COLS,),
            in_specs=[pl.BlockSpec((BLK, DIM), lambda j, *_: (0, 0))] * 4
            + [
                pl.BlockSpec((1, DIM), lambda j, *_: (0, 0)),
                pl.BlockSpec((DIM, FWD_COLS), lambda j, *_: (0, j)),
            ],
            out_specs=[
                pl.BlockSpec((4 * BLK, DIM), lambda j, *_: (0, 0)),
                pl.BlockSpec((4, 2, BLK), lambda j, *_: (0, 0, 0)),
            ],
            scratch_shapes=[
                pltpu.VMEM((4 * BLK, 128), f32),
                pltpu.VMEM((4 * BLK, 128), f32),
                pltpu.VMEM((SUB, FWD_COLS), f32),
            ],
        ),
        out_shape=[
            jax.ShapeDtypeStruct((4 * BLK, DIM), bf16),
            jax.ShapeDtypeStruct((4, 2, BLK), f32),
        ],
        compiler_params=pltpu.CompilerParams(dimension_semantics=("arbitrary",)),
        cost_estimate=pl.CostEstimate(
            flops=2 * 4 * BLK * DIM * vocab, bytes_accessed=2 * DIM * vocab + 10 * BLK * DIM * 4, transcendentals=4 * BLK * vocab
        ),
        name="fwd_stats",
    )(offs, span, ntiles, *blocks, g, w)


def grad_logits(z, aux, col0):
    target = aux[:, 2:3].astype(i32) - col0
    hot = lax.broadcasted_iota(i32, z.shape, 1) == target
    p = jnp.exp(z - aux[:, 0:1])
    dz = (jnp.where(hot, p - 1.0, p) * aux[:, 1:2]).astype(bf16)
    return dz, hot


def dn_kernel(offs_ref, span_ref, kept_ref, nt_ref, col_ref, n_ref, aux_ref, w_ref, dn_ref, tl_ref, acc_ref, auxc_ref, dz_ref):
    j = pl.program_id(0)

    @pl.when(j == 0)
    def _():
        acc_ref[...] = jnp.zeros_like(acc_ref)
        auxc_ref[...] = jnp.zeros_like(auxc_ref)
        tl_ref[...] = jnp.zeros_like(tl_ref)
        for b in range(4):
            place_masked(auxc_ref, offs_ref[b], span_ref[b], aux_columns(aux_ref[b]))

    col0 = col_ref[0] + j * DN_COLS

    def tile(i, carry):
        rows = pl.ds(pl.multiple_of(i * BLK, BLK), BLK)
        aux = auxc_ref[rows, :]
        n = n_ref[rows, :]
        found = jnp.zeros((BLK, 128), f32)
        for c in range(DN_COLS // 512):
            z = jnp.dot(n, w_ref[:, c * 512 : (c + 1) * 512], preferred_element_type=f32)
            dz, hot = grad_logits(z, aux, col0 + c * 512)
            dz_ref[:, c * 512 : (c + 1) * 512] = dz
            picked = jnp.where(hot, z, 0.0)
            for k in range(4):
                found += picked[:, k * 128 : (k + 1) * 128]
        tl_ref[...] += jnp.sum((found * aux[:, 1:2]).reshape(BLK // 8, 8, 128), axis=0)
        acc_ref[rows, :] += lax.dot_general(dz_ref[...], w_ref[...], (((1,), (1,)), ((), ())), preferred_element_type=f32)
        return carry

    lax.fori_loop(0, nt_ref[0], tile, 0)

    @pl.when(j == pl.num_programs(0) - 1)
    def _():
        for b in range(4):
            got = acc_ref[pl.ds(pl.multiple_of(offs_ref[b], ALIGN), BLK), :]
            live = lax.broadcasted_iota(i32, (BLK, 1), 0) < kept_ref[b]
            dn_ref[pl.ds(b * BLK, BLK), :] = jnp.where(live, got, 0.0)


def backward_dn(offs, span, kept, ntiles, col0, n_row, aux_row, w):
    vocab = w.shape[1]
    return pl.pallas_call(
        dn_kernel,
        grid_spec=pltpu.PrefetchScalarGridSpec(
            num_scalar_prefetch=5,
            grid=(vocab // DN_COLS,),
            in_specs=[
                pl.BlockSpec((4 * BLK, DIM), lambda j, *_: (0, 0)),
                pl.BlockSpec((4, 8, BLK), lambda j, *_: (0, 0, 0)),
                pl.BlockSpec((DIM, DN_COLS), lambda j, *_: (0, j)),
            ],
            out_specs=[
                pl.BlockSpec((4 * BLK, DIM), lambda j, *_: (0, 0)),
                pl.BlockSpec((8, 128), lambda j, *_: (0, 0)),
            ],
            scratch_shapes=[
                pltpu.VMEM((4 * BLK, DIM), f32),
                pltpu.VMEM((4 * BLK, 128), f32),
                pltpu.VMEM((BLK, DN_COLS), bf16),
            ],
        ),
        out_shape=[
            jax.ShapeDtypeStruct((4 * BLK, DIM), f32),
            jax.ShapeDtypeStruct((8, 128), f32),
        ],
        compiler_params=pltpu.CompilerParams(dimension_semantics=("arbitrary",)),
        cost_estimate=pl.CostEstimate(
            flops=4 * 4 * BLK * DIM * vocab, bytes_accessed=2 * DIM * vocab + 6 * BLK * DIM * 4, transcendentals=4 * BLK * vocab
        ),
        name="backward_dn",
    )(offs, span, kept, ntiles, col0, n_row, aux_row, w)


def gather_kernel(offs_ref, xh_ref, g_ref, aux_ref, n_hbm, aux_hbm, n_ref, auxc_ref, sems):
    step = pl.program_id(0)
    last = pl.num_programs(0) - 1
    tokens = n_ref.shape[0]
    chunks = tokens // DW_TOK

    @pl.when(step == 0)
    def _():
        def clear(i, carry):
            rows = pl.ds(pl.multiple_of(i * BLK, BLK), BLK)
            n_ref[rows, :] = jnp.zeros((BLK, DIM), bf16)
            auxc_ref[rows, :] = jnp.zeros((BLK, 128), f32)
            return carry

        lax.fori_loop(0, tokens // BLK, clear, 0)

    def copies(q):
        rows = pl.ds(q * DW_TOK, DW_TOK)
        return (
            pltpu.make_async_copy(n_ref.at[rows, :], n_hbm.at[rows, :], sems.at[q, 0]),
            pltpu.make_async_copy(auxc_ref.at[rows, :], aux_hbm.at[rows, :], sems.at[q, 1]),
        )

    def block(k, carry):
        off = pl.multiple_of(offs_ref[step * 4 + k], ALIGN)
        src = pl.ds(pl.multiple_of(k * BLK, BLK), BLK)
        n_ref[pl.ds(off, BLK), :] = (xh_ref[src, :] * g_ref[...]).astype(bf16)
        auxc_ref[pl.ds(off, BLK), :] = aux_columns(aux_ref[k])
        return carry

    lax.fori_loop(0, 4, block, 0)
    before, after = offs_ref[step * 4], offs_ref[step * 4 + 4]
    reach = jnp.where(step == last, after + DW_TOK - 1, after)
    for q in range(chunks):
        end = (q + 1) * DW_TOK

        @pl.when((end <= reach) & (end > before))
        def _():
            for copy in copies(q):
                copy.start()

    @pl.when(step == last)
    def _():
        for q in range(chunks):

            @pl.when(q * DW_TOK < after)
            def _():
                for copy in copies(q):
                    copy.wait()


def gather_tokens(offs, xh_all, g, aux_all):
    blocks = aux_all.shape[0]
    tokens = blocks * BLK
    anywhere = pl.BlockSpec(memory_space=pl.ANY)
    return pl.pallas_call(
        gather_kernel,
        grid_spec=pltpu.PrefetchScalarGridSpec(
            num_scalar_prefetch=1,
            grid=(blocks // 4,),
            in_specs=[
                pl.BlockSpec((4 * BLK, DIM), lambda b, *_: (b, 0)),
                pl.BlockSpec((1, DIM), lambda b, *_: (0, 0)),
                pl.BlockSpec((4, 8, BLK), lambda b, *_: (b, 0, 0)),
            ],
            out_specs=[anywhere, anywhere],
            scratch_shapes=[
                pltpu.VMEM((tokens, DIM), bf16),
                pltpu.VMEM((tokens, 128), f32),
                pltpu.SemaphoreType.DMA((tokens // DW_TOK, 2)),
            ],
        ),
        out_shape=[
            jax.ShapeDtypeStruct((tokens, DIM), bf16),
            jax.ShapeDtypeStruct((tokens, 128), f32),
        ],
        compiler_params=pltpu.CompilerParams(dimension_semantics=("arbitrary",), vmem_limit_bytes=56 << 20),
        cost_estimate=pl.CostEstimate(flops=2 * tokens * DIM, bytes_accessed=6 * tokens * DIM, transcendentals=0),
        name="gather_tokens",
    )(offs, xh_all, g, aux_all)


def dw_kernel(merge, place_ref, nt_ref, n_hbm, aux_hbm, w_ref, *rest):
    out_ref, all_hbm, nbuf, abuf, dz_ref, sems, own_sems = rest[-7 - 2 * merge : len(rest) - 2 * merge]
    s = pl.program_id(0)
    steps = nt_ref[0]

    def fetch(i, slot):
        rows = pl.ds(pl.multiple_of(i * DW_TOK, DW_TOK), DW_TOK)
        return (
            pltpu.make_async_copy(n_hbm.at[rows, :], nbuf.at[slot], sems.at[slot, 0]),
            pltpu.make_async_copy(aux_hbm.at[rows, :], abuf.at[slot], sems.at[slot, 1]),
        )

    def keep(step):
        cols = pl.ds(pl.multiple_of((place_ref[0] + step) * DW_COLS, DW_COLS), DW_COLS)
        return pltpu.make_async_copy(out_ref, all_hbm.at[:, cols], own_sems.at[step])

    if merge:
        recv_hbm, (mbuf, msems) = rest[-10], rest[-2:]
        cols = pl.ds(pl.multiple_of(place_ref[2], DW_COLS), DW_COLS * DW_STEPS)
        merge_in = pltpu.make_async_copy(recv_hbm, mbuf, msems.at[0])
        merge_out = pltpu.make_async_copy(mbuf, all_hbm.at[:, cols], msems.at[1])

    @pl.when(s == 0)
    def _():
        for copy in fetch(0, 0):
            copy.start()
        if merge:
            merge_in.start()

    out_ref[...] = jnp.zeros_like(out_ref)
    col0 = place_ref[1] + s * DW_COLS

    def tile(i, carry):
        g = s * steps + i
        slot = lax.rem(g, 2)

        @pl.when(g + 1 < DW_STEPS * steps)
        def _():
            for copy in fetch(jnp.where(i + 1 < steps, i + 1, 0), 1 - slot):
                copy.start()

        for copy in fetch(i, slot):
            copy.wait()
        for u in range(DW_TOK // SUB):
            rows = pl.ds(u * SUB, SUB)
            z = jnp.dot(nbuf[slot, rows, :], w_ref[...], preferred_element_type=f32)
            dz_ref[rows, :], _ = grad_logits(z, abuf[slot, rows, :], col0)
        out_ref[...] += lax.dot_general(nbuf[slot], dz_ref[...], (((0,), (0,)), ((), ())), preferred_element_type=f32)
        return carry

    lax.fori_loop(0, steps, tile, 0)
    for step in range(DW_STEPS):

        @pl.when(s == step)
        def _():
            keep(step).start()
            if merge and step == 0:
                merge_in.wait()
                merge_out.start()
            if step == DW_STEPS - 1:
                for done in range(DW_STEPS):
                    keep(done).wait()
                if merge:
                    merge_out.wait()


def weight_grad(place, ntiles, n_all, aux_all, w, whole, recv):
    tokens, vocab = n_all.shape[0], w.shape[1]
    width = DW_COLS * DW_STEPS
    anywhere = pl.BlockSpec(memory_space=pl.ANY)
    held = [a for a in (whole, recv) if a is not None]
    merge = recv is not None
    scratch = [
        pltpu.VMEM((2, DW_TOK, DIM), bf16),
        pltpu.VMEM((2, DW_TOK, 128), f32),
        pltpu.VMEM((DW_TOK, DW_COLS), bf16),
        pltpu.SemaphoreType.DMA((2, 2)),
        pltpu.SemaphoreType.DMA((DW_STEPS,)),
    ]
    if merge:
        scratch += [pltpu.VMEM((DIM, width), f32), pltpu.SemaphoreType.DMA((2,))]
    return pl.pallas_call(
        functools.partial(dw_kernel, merge),
        grid_spec=pltpu.PrefetchScalarGridSpec(
            num_scalar_prefetch=2,
            grid=(DW_STEPS,),
            in_specs=[anywhere, anywhere, pl.BlockSpec((DIM, DW_COLS), lambda s, place, nt: (0, place[0] + s))]
            + [anywhere] * len(held),
            out_specs=[pl.BlockSpec((DIM, DW_COLS), lambda s, *_: (0, s)), anywhere],
            scratch_shapes=scratch,
        ),
        out_shape=[
            jax.ShapeDtypeStruct((DIM, width), f32),
            jax.ShapeDtypeStruct((DIM, vocab), f32),
        ],
        input_output_aliases={} if whole is None else {5: 1},
        compiler_params=pltpu.CompilerParams(dimension_semantics=("arbitrary",)),
        cost_estimate=pl.CostEstimate(
            flops=2 * tokens * DIM * width, bytes_accessed=2 * tokens * DIM + 8 * DIM * width, transcendentals=tokens * width // 2
        ),
        name="weight_grad",
    )(place, ntiles.reshape(1), n_all, aux_all, w, *held)


def solution(mesh):
    dp_count, vp_count = mesh.shape["dp"], mesh.shape["vp"]
    everyone = (dp_count, vp_count)

    def local_step(hidden, targets, loss_mask, norm_scale, w_head):
        vocab = w_head.shape[1]
        dp, vp = lax.axis_index("dp"), lax.axis_index("vp")
        g = norm_scale.reshape(1, DIM)

        mask = loss_mask[0]
        idx = lax.iota(i32, BLK)
        before = jnp.sum(jnp.where(idx[None, :] < idx[:, None], mask[None, :], 0), axis=1)
        kept = jnp.sum(mask)
        pos = jnp.where(mask == 1, before, kept + idx - before)
        perm = pos[None, :] == idx[:, None]
        x_sorted = jnp.dot(perm.astype(bf16), hidden[0], preferred_element_type=f32)
        t_sorted = jnp.sum(jnp.where(perm, targets[0][None, :], 0), axis=1)
        inv_rms = lax.rsqrt(jnp.mean(x_sorted * x_sorted, axis=-1, keepdims=True) + EPS)
        x_hat = x_sorted * inv_rms

        core_pairs = [(v, v ^ 1) for v in range(vp_count)]
        x_pairs = [(v, v ^ 2) for v in range(vp_count)]
        from_x = lax.ppermute(x_hat, "vp", x_pairs)
        from_core = lax.ppermute(x_hat, "vp", core_pairs)
        xh_all = lax.all_gather(x_hat, ("dp", "vp"), axis=0, tiled=True)
        info = jnp.concatenate([t_sorted.astype(f32).reshape(4, 128), jnp.full((4, 128), kept.astype(f32))])
        info = tiny_gather(info, everyone, 1)
        from_x_core = lax.ppermute(from_x, "vp", core_pairs)
        blocks = (x_hat, from_core, from_x, from_x_core)

        t_all = info[:, :4].reshape(dp_count * vp_count, BLK)
        kept_all = info[:, 4, 0].astype(i32)
        span = (kept_all + ALIGN - 1) // ALIGN * ALIGN
        ends = jnp.cumsum(span)
        offs_all = jnp.concatenate([jnp.zeros((1,), i32), ends])
        total = ends[-1]
        weight = 1.0 / jnp.sum(kept_all).astype(f32)
        first = dp * vp_count
        kept_row = lax.dynamic_slice(kept_all, (first,), (vp_count,))
        offs_row = lax.dynamic_slice(offs_all, (first,), (vp_count,))
        span_row = lax.dynamic_slice(span, (first,), (vp_count,))
        offs_row = offs_row - offs_row[0]
        nt_row = ((jnp.sum(span_row) + BLK - 1) // BLK).reshape(1)
        nt_all = jnp.maximum((total + DW_TOK - 1) // DW_TOK, 1)

        table = jnp.stack([jnp.arange(vp_count) ^ v for v in range(vp_count)])
        mine = lax.dynamic_slice(table, (vp, 0), (1, vp_count))[0]
        pick = (mine[:, None] == jnp.arange(vp_count)[None, :]).astype(i32)
        offs_mine = jnp.sum(pick * offs_row[None, :], axis=1)
        span_mine = jnp.sum(pick * span_row[None, :], axis=1)

        n_row, stats = forward_stats(offs_mine, span_mine, nt_row, blocks, g, w_head)
        stats = lax.all_gather(stats, "vp", axis=0)
        stats = jnp.stack([jnp.stack([stats[v, b ^ v] for b in range(vp_count)]) for v in range(vp_count)])
        row_max = jnp.max(stats[:, :, 0], axis=0)
        row_sum = jnp.sum(stats[:, :, 1] * jnp.exp(stats[:, :, 0] - row_max), axis=0)
        lse_row = row_max + jnp.log(row_sum)
        lse_row = jnp.where(idx[None, :] < kept_row[:, None], lse_row, DROPPED)
        w_row = jnp.where(idx[None, :] < kept_row[:, None], weight, 0.0)
        t_row = lax.dynamic_slice(t_all, (first, 0), (vp_count, BLK))
        none = jnp.zeros_like(w_row)
        aux_row = jnp.stack([lse_row, w_row, t_row] + [none] * 5, axis=1)

        dn_part, t_part = backward_dn(
            offs_row, span_row, kept_row, nt_row, (vp * vocab).reshape(1), n_row, aux_row, w_head
        )
        d_normed = lax.psum_scatter(dn_part, "vp", scatter_dimension=0, tiled=True)

        lse_own = lax.dynamic_slice(lse_row, (vp, 0), (1, BLK))[0]
        lse_own, t_part = lax.optimization_barrier((lse_own, t_part))
        lse_all = tiny_gather(jnp.concatenate([lse_own.reshape(4, 128), jnp.zeros((4, 128), f32)]), everyone, 2)
        lse_all = lse_all[:, :4].reshape(dp_count * vp_count, BLK)
        w_all = jnp.where(idx[None, :] < kept_all[:, None], weight, 0.0)
        none = jnp.zeros_like(w_all)
        aux_all = jnp.stack([lse_all, w_all, t_all] + [none] * 5, axis=1)
        n_all, auxc_all = gather_tokens(offs_all, xh_all, g, aux_all)

        d_scale = jnp.sum(d_normed * x_hat, axis=0)
        e = d_normed * norm_scale
        d_x = inv_rms * (e - x_hat * jnp.mean(e * x_hat, axis=-1, keepdims=True))
        back = perm.astype(bf16).T
        d_x = jnp.dot(back, d_x.astype(bf16), preferred_element_type=f32).astype(bf16)
        loss_part = weight * jnp.sum(jnp.where(idx < kept, lse_own, 0.0)) - jnp.sum(t_part)
        parts = jnp.concatenate([d_scale.reshape(6, 128), jnp.full((2, 128), loss_part, f32)])
        parts = jnp.sum(tiny_gather(parts, everyone, 3), axis=0)

        half, quarter, width = vocab // 2, vocab // 4, DW_COLS * DW_STEPS
        y_pos, z_pos = dp % 2, (dp // 2) % 2
        y_pairs = [(d, d ^ 1) for d in range(dp_count)]
        z_pairs = [(d, d ^ 2) for d in range(dp_count)]
        jobs = [
            (base + where * quarter + c * width, base + (1 - where) * quarter + c * width, pairs)
            for c in range(quarter // width)
            for base, where, pairs in ((0, y_pos, y_pairs), (half, z_pos, z_pairs))
        ]
        whole, moved = None, []
        for k, (col, other, pairs) in enumerate(jobs):
            if k == len(jobs) - 2:
                n_all, parts, d_x = lax.optimization_barrier((n_all, parts, d_x))
            ahead = moved[k - LAG] if k >= LAG else (0, None)
            place = jnp.stack([col // DW_COLS, vp * vocab + col, ahead[0]]).astype(i32)
            chunk, whole = weight_grad(place, nt_all, n_all, auxc_all, w_head, whole, ahead[1])
            moved.append((other, lax.ppermute(chunk, "dp", pairs)))
        for other, chunk in moved[-LAG:]:
            whole = lax.dynamic_update_slice(whole, chunk, (0, other))
        return parts[6, 0], d_x[None], whole, parts[:6].reshape(DIM)

    return jax.shard_map(
        local_step,
        mesh=mesh,
        in_specs=(P("dp", "vp", None), P("dp", "vp"), P("dp", "vp"), P(None), P(None, "vp")),
        out_specs=(P(), P("dp", "vp", None), P(None, "vp"), P(None)),
        check_vma=False,
    )
```

```python
import functools

import jax
import jax.numpy as jnp
from jax import lax
from jax.experimental import pallas as pl
from jax.experimental.pallas import tpu as pltpu
from jax.sharding import PartitionSpec as P


EPS = 1e-5
BLK = 512
DIM = 768
ALIGN = 16
FWD_COLS = 2048
FWD_GROUP = 512
DN_COLS = 2048
DW_TOK = 1024
DW_GROUP = 1024
SUB = 256
Y_WIDTHS = (1024, 1024, 1024, 512, 512)
Z_WIDTHS = (1024, 1024, 1024, 512, 256, 256)
LAG = 4
DROPPED = 1e30
LOG2E = 1.4426950408889634


f32, bf16, i32 = jnp.float32, jnp.bfloat16, jnp.int32


def tiny_gather_kernel(dp_count, vp_count, x_ref, out_ref, send_sems, recv_sems):
    count = dp_count * vp_count
    me = lax.axis_index("dp") * vp_count + lax.axis_index("vp")
    barrier = pltpu.get_barrier_semaphore()

    def peer(k):
        other = lax.rem(me + k, count)
        return (other // vp_count, lax.rem(other, vp_count))

    for k in range(1, count):
        pl.semaphore_signal(barrier, inc=1, device_id=peer(k), device_id_type=pl.DeviceIdType.MESH)
    pl.semaphore_wait(barrier, count - 1)
    copies = [
        pltpu.make_async_remote_copy(
            src_ref=x_ref,
            dst_ref=out_ref.at[me],
            send_sem=send_sems.at[k - 1],
            recv_sem=recv_sems.at[k - 1],
            device_id=peer(k),
            device_id_type=pl.DeviceIdType.MESH,
        )
        for k in range(1, count)
    ]
    for copy in copies:
        copy.start()
    out_ref[me] = x_ref[...]
    for copy in copies:
        copy.wait()


def tiny_gather(x, mesh_shape, collective_id):
    dp_count, vp_count = mesh_shape
    count = dp_count * vp_count
    return pl.pallas_call(
        functools.partial(tiny_gather_kernel, dp_count, vp_count),
        out_shape=jax.ShapeDtypeStruct((count, 8, 128), f32),
        in_specs=[pl.BlockSpec(memory_space=pltpu.VMEM)],
        out_specs=pl.BlockSpec(memory_space=pltpu.VMEM),
        scratch_shapes=[pltpu.SemaphoreType.DMA((count - 1,)), pltpu.SemaphoreType.DMA((count - 1,))],
        compiler_params=pltpu.CompilerParams(collective_id=collective_id, has_side_effects=True),
        name="tiny_gather",
    )(x)


def place_masked(dst, off, span, new):
    rows = pl.ds(pl.multiple_of(off, ALIGN), BLK)
    live = lax.broadcasted_iota(i32, (BLK, 1), 0) < span
    dst[rows, :] = jnp.where(live, new, dst[rows, :].astype(f32)).astype(dst.dtype)


def aux_columns(aux):
    pad = jnp.zeros((120, aux.shape[1]), f32)
    return jnp.concatenate([aux, pad], axis=0).T


def fwd_kernel(xa, xb, g_ref, w_ref, n_ref, st_ref, m_ref, s_ref, za_ref, zb_ref):
    j = pl.program_id(0)
    groups = FWD_COLS // FWD_GROUP
    bufs = (za_ref, zb_ref)

    @pl.when(j == 0)
    def _():
        m_ref[...] = jnp.full_like(m_ref, -DROPPED)
        s_ref[...] = jnp.zeros_like(s_ref)
        zb_ref[...] = jnp.full_like(zb_ref, -DROPPED)
        for k, x_ref in enumerate((xa, xb)):
            n_ref[pl.ds(k * BLK, BLK), :] = (x_ref[...] * g_ref[...]).astype(bf16)

    def absorb(row, z_ref):
        for r in range(0, BLK, 8):
            rows = pl.ds(pl.multiple_of(row + r, 8), 8)
            parts = [z_ref[r : r + 8, k * 128 : (k + 1) * 128] for k in range(FWD_GROUP // 128)]
            m_old = m_ref[rows, :]
            m_new = jnp.maximum(functools.reduce(jnp.maximum, parts), m_old)
            total = functools.reduce(jnp.add, [jnp.exp(part - m_new) for part in parts])
            s_ref[rows, :] = s_ref[rows, :] * jnp.exp(m_old - m_new) + total
            m_ref[rows, :] = m_new

    def tile(i, carry):
        row = pl.multiple_of(i * BLK, BLK)
        n = n_ref[pl.ds(row, BLK), :]
        for c in range(groups):
            cols = pl.ds(c * FWD_GROUP, FWD_GROUP)
            bufs[c % 2][...] = jnp.dot(n, w_ref[:, cols], preferred_element_type=f32)
            absorb(row if c else pl.multiple_of((1 - i) * BLK, BLK), bufs[(c + 1) % 2])
        return carry

    lax.fori_loop(0, 2, tile, 0)

    @pl.when(j == pl.num_programs(0) - 1)
    def _():
        absorb(BLK, zb_ref)
        for k in range(2):
            rows = pl.ds(k * BLK, BLK)
            m_lane = m_ref[rows, :]
            m = jnp.max(m_lane, axis=1, keepdims=True)
            s = jnp.sum(s_ref[rows, :] * jnp.exp(m_lane - m), axis=1, keepdims=True)
            st_ref[k, 0:1, :] = jnp.broadcast_to(m, (BLK, 128)).T[0:1, :]
            st_ref[k, 1:2, :] = jnp.broadcast_to(s, (BLK, 128)).T[0:1, :]


def forward_stats(xa, xb, g, w):
    vocab = w.shape[1]
    return pl.pallas_call(
        fwd_kernel,
        grid=(vocab // FWD_COLS,),
        in_specs=[pl.BlockSpec((BLK, DIM), lambda j: (0, 0))] * 2
        + [
            pl.BlockSpec((1, DIM), lambda j: (0, 0)),
            pl.BlockSpec((DIM, FWD_COLS), lambda j: (0, j)),
        ],
        out_specs=[
            pl.BlockSpec((2 * BLK, DIM), lambda j: (0, 0)),
            pl.BlockSpec((2, 2, BLK), lambda j: (0, 0, 0)),
        ],
        scratch_shapes=[
            pltpu.VMEM((2 * BLK, 128), f32),
            pltpu.VMEM((2 * BLK, 128), f32),
            pltpu.VMEM((BLK, FWD_GROUP), f32),
            pltpu.VMEM((BLK, FWD_GROUP), f32),
        ],
        out_shape=[
            jax.ShapeDtypeStruct((2 * BLK, DIM), bf16),
            jax.ShapeDtypeStruct((2, 2, BLK), f32),
        ],
        compiler_params=pltpu.CompilerParams(dimension_semantics=("arbitrary",)),
        cost_estimate=pl.CostEstimate(
            flops=2 * 2 * BLK * DIM * vocab, bytes_accessed=2 * DIM * vocab + 5 * BLK * DIM * 4, transcendentals=2 * BLK * vocab
        ),
        name="fwd_stats",
    )(xa, xb, g, w)


def grad_logits(z, aux, col0):
    target = aux[:, 2:3].astype(i32) - col0
    hot = lax.broadcasted_iota(i32, z.shape, 1) == target
    p = jnp.exp2(z * LOG2E - aux[:, 0:1])
    return jnp.where(hot, p - aux[:, 1:2], p).astype(bf16), hot


def dn_kernel(
    offs_ref, span_ref, kept_ref, mine_ref, nt_ref, col_ref, na_ref, nb_ref, aux_ref, w_ref, dn_ref, tl_ref, acc_ref, auxc_ref, n_ref, dz_ref
):
    j = pl.program_id(0)

    @pl.when(j == 0)
    def _():
        acc_ref[...] = jnp.zeros_like(acc_ref)
        auxc_ref[...] = jnp.zeros_like(auxc_ref)
        tl_ref[...] = jnp.zeros_like(tl_ref)
        n_ref[...] = jnp.zeros_like(n_ref)
        for b in range(4):
            place_masked(auxc_ref, offs_ref[b], span_ref[b], aux_columns(aux_ref[b]))
            src = (na_ref, na_ref, nb_ref, nb_ref)[b][pl.ds(b % 2 * BLK, BLK), :].astype(f32)
            place_masked(n_ref, offs_ref[mine_ref[b]], span_ref[mine_ref[b]], src)

    col0 = col_ref[0] + j * DN_COLS

    def tile(i, carry):
        rows = pl.ds(pl.multiple_of(i * BLK, BLK), BLK)
        aux = auxc_ref[rows, :]
        n = n_ref[rows, :]
        found = jnp.zeros((BLK, 128), f32)
        for c in range(DN_COLS // 512):
            z = jnp.dot(n, w_ref[:, c * 512 : (c + 1) * 512], preferred_element_type=f32)
            dz, hot = grad_logits(z, aux, col0 + c * 512)
            dz_ref[:, c * 512 : (c + 1) * 512] = dz
            picked = jnp.where(hot, z, 0.0)
            for k in range(4):
                found += picked[:, k * 128 : (k + 1) * 128]
        tl_ref[...] += jnp.sum((found * aux[:, 1:2]).reshape(BLK // 8, 8, 128), axis=0)
        acc_ref[rows, :] += lax.dot_general(dz_ref[...], w_ref[...], (((1,), (1,)), ((), ())), preferred_element_type=f32)
        return carry

    lax.fori_loop(0, nt_ref[0], tile, 0)

    @pl.when(j == pl.num_programs(0) - 1)
    def _():
        for b in range(4):
            got = acc_ref[pl.ds(pl.multiple_of(offs_ref[b], ALIGN), BLK), :]
            live = lax.broadcasted_iota(i32, (BLK, 1), 0) < kept_ref[b]
            dn_ref[pl.ds(b * BLK, BLK), :] = jnp.where(live, got, 0.0)


def backward_dn(offs, span, kept, mine, ntiles, col0, n_near, n_far, aux_row, w):
    vocab = w.shape[1]
    return pl.pallas_call(
        dn_kernel,
        grid_spec=pltpu.PrefetchScalarGridSpec(
            num_scalar_prefetch=6,
            grid=(vocab // DN_COLS,),
            in_specs=[
                pl.BlockSpec((2 * BLK, DIM), lambda j, *_: (0, 0)),
                pl.BlockSpec((2 * BLK, DIM), lambda j, *_: (0, 0)),
                pl.BlockSpec((4, 8, BLK), lambda j, *_: (0, 0, 0)),
                pl.BlockSpec((DIM, DN_COLS), lambda j, *_: (0, j)),
            ],
            out_specs=[
                pl.BlockSpec((4 * BLK, DIM), lambda j, *_: (0, 0)),
                pl.BlockSpec((8, 128), lambda j, *_: (0, 0)),
            ],
            scratch_shapes=[
                pltpu.VMEM((4 * BLK, DIM), f32),
                pltpu.VMEM((4 * BLK, 128), f32),
                pltpu.VMEM((4 * BLK, DIM), bf16),
                pltpu.VMEM((BLK, DN_COLS), bf16),
            ],
        ),
        out_shape=[
            jax.ShapeDtypeStruct((4 * BLK, DIM), f32),
            jax.ShapeDtypeStruct((8, 128), f32),
        ],
        compiler_params=pltpu.CompilerParams(dimension_semantics=("arbitrary",)),
        cost_estimate=pl.CostEstimate(
            flops=4 * 4 * BLK * DIM * vocab, bytes_accessed=2 * DIM * vocab + 6 * BLK * DIM * 4, transcendentals=4 * BLK * vocab
        ),
        name="backward_dn",
    )(offs, span, kept, mine, ntiles, col0, n_near, n_far, aux_row, w)


def dw_tile(load, aux, w_ref, dz_ref, acc_ref, col0):
    width = acc_ref.shape[1]
    group = min(width, DW_GROUP)
    sub = SUB if width > 256 else 2 * SUB
    for c in range(width // group):
        cols = pl.ds(c * group, group)
        for u in range(DW_TOK // sub):
            rows = pl.ds(u * sub, sub)
            z = jnp.dot(load(u * sub, sub), w_ref[:, cols], preferred_element_type=f32)
            dz_ref[rows, cols], _ = grad_logits(z, aux(u * sub, sub), col0 + c * group)
        acc_ref[:, cols] += lax.dot_general(
            load(0, DW_TOK), dz_ref[:, cols], (((0,), (0,)), ((), ())), preferred_element_type=f32
        )


def first_kernel(final, offs_ref, place_ref, xh_ref, aux_ref, g_ref, w_ref, *rest):
    n_hbm, aux_hbm, acc_ref, n_img, aux_img, dz_ref, sems = rest[-7:]
    step = pl.program_id(0)
    last = pl.num_programs(0) - 1
    half = BLK // 2
    base = offs_ref[0] // DW_TOK
    end = offs_ref[offs_ref.shape[0] - 1]

    def images(t):
        rows = pl.ds(pl.multiple_of((t - base) * DW_TOK, DW_TOK), DW_TOK)
        return n_img.at[rows, :], aux_img.at[rows, :]

    def places(t):
        rows = pl.ds(pl.multiple_of(t * DW_TOK, DW_TOK), DW_TOK)
        return n_hbm.at[rows, :], aux_hbm.at[rows, :]

    def copies(t):
        return [pltpu.make_async_copy(a, b, sems.at[k]) for k, (a, b) in enumerate(zip(images(t), places(t)))]

    @pl.when(step == 0)
    def _():
        if final:
            acc_ref[...] = rest[2][...]
            loads = [pltpu.make_async_copy(b, a, sems.at[k]) for k, (a, b) in enumerate(zip(images(base), places(base)))]
            for copy in loads:
                copy.start()
            for copy in loads:
                copy.wait()
        else:
            acc_ref[...] = jnp.zeros_like(acc_ref)

    for k in range(4):
        off = pl.multiple_of(offs_ref[step * 4 + k] - base * DW_TOK, ALIGN)
        n_img[pl.ds(off, half), :] = (xh_ref[k] * g_ref[...]).astype(bf16)
        aux_img[pl.ds(off, half), :] = aux_columns(aux_ref[k])

    @pl.when(step == last)
    def _():
        rows = pl.ds(pl.multiple_of(end - base * DW_TOK, ALIGN), DW_TOK)
        n_img[rows, :] = jnp.zeros((DW_TOK, DIM), bf16)
        aux_img[rows, :] = jnp.zeros((DW_TOK, 128), f32)

    full = offs_ref[step * 4 + 4] // DW_TOK
    stop = jnp.where(step == last, (end + DW_TOK - 1) // DW_TOK, full) if final else full

    def tile(t, carry):
        for copy in copies(t):
            copy.start()
        row = (t - base) * DW_TOK

        def rows(start, size):
            return pl.ds(pl.multiple_of(row, DW_TOK) + start, size)

        dw_tile(
            lambda *r: n_img[rows(*r), :], lambda *r: aux_img[rows(*r), :], w_ref, dz_ref, acc_ref, place_ref[1]
        )
        return carry

    lax.fori_loop(offs_ref[step * 4] // DW_TOK, stop, tile, 0)

    @pl.when(step == last)
    def _():
        if not final:
            for copy in copies(full):
                copy.start()

        def drain(t, carry):
            for copy in copies(t):
                copy.wait()
            return carry

        lax.fori_loop(base, stop if final else full + 1, drain, 0)


def first_columns(half, offs, place, xh_half, aux_all, g, w, before):
    blocks = aux_all.shape[0]
    tokens = blocks * BLK
    image = tokens // 2 + 2 * DW_TOK
    width = Y_WIDTHS[0]
    anywhere = pl.BlockSpec(memory_space=pl.ANY)
    whole_chunk = pl.BlockSpec((DIM, width), lambda b, *_: (0, 0))
    final = before is not None
    return pl.pallas_call(
        functools.partial(first_kernel, final),
        grid_spec=pltpu.PrefetchScalarGridSpec(
            num_scalar_prefetch=2,
            grid=(blocks // 4,),
            in_specs=[
                pl.BlockSpec((4, BLK // 2, DIM), lambda b, *_: (b, 0, 0)),
                pl.BlockSpec((4, 8, BLK // 2), lambda b, *_: (b, 0, half)),
                pl.BlockSpec((1, DIM), lambda b, *_: (0, 0)),
                pl.BlockSpec((DIM, width), lambda b, offs, place: (0, place[0])),
            ]
            + ([anywhere, anywhere, whole_chunk] if final else []),
            out_specs=[anywhere, anywhere, whole_chunk],
            scratch_shapes=[
                pltpu.VMEM((image, DIM), bf16),
                pltpu.VMEM((image, 128), f32),
                pltpu.VMEM((DW_TOK, width), bf16),
                pltpu.SemaphoreType.DMA((2,)),
            ],
        ),
        out_shape=[
            jax.ShapeDtypeStruct((tokens, DIM), bf16),
            jax.ShapeDtypeStruct((tokens, 128), f32),
            jax.ShapeDtypeStruct((DIM, width), f32),
        ],
        input_output_aliases={6: 0, 7: 1} if final else {},
        compiler_params=pltpu.CompilerParams(dimension_semantics=("arbitrary",), vmem_limit_bytes=60 << 20),
        cost_estimate=pl.CostEstimate(
            flops=tokens * DIM * width, bytes_accessed=4 * tokens * DIM, transcendentals=tokens * width // 4
        ),
        name="first_columns",
    )(offs, place, xh_half.reshape(blocks, BLK // 2, DIM), aux_all, g, w, *(before or ()))


def dw_kernel(merges, place_ref, nt_ref, n_hbm, aux_hbm, w_ref, *rest):
    inputs, rest = rest[: -(6 + merges + 1)], rest[-(6 + merges + 1) :]
    out_ref, all_hbm, nbuf, abuf, dz_ref, sems = rest[:6]
    mbufs, out_sems = rest[6:-1], rest[-1]
    steps = nt_ref[0]

    def fetch(i, slot):
        rows = pl.ds(pl.multiple_of(i * DW_TOK, DW_TOK), DW_TOK)
        return (
            pltpu.make_async_copy(n_hbm.at[rows, :], nbuf.at[slot], sems.at[slot, 0]),
            pltpu.make_async_copy(aux_hbm.at[rows, :], abuf.at[slot], sems.at[slot, 1]),
        )

    def put(ref, col, sem):
        return pltpu.make_async_copy(ref, all_hbm.at[:, pl.ds(pl.multiple_of(col, 128), ref.shape[1])], sem)

    for copy in fetch(0, 0):
        copy.start()
    moves_in = [pltpu.make_async_copy(src, mbuf, out_sems.at[k, 0]) for k, (src, mbuf) in enumerate(zip(inputs[-merges:], mbufs))]
    moves_out = [put(mbuf, place_ref[3 + k], out_sems.at[k, 1]) for k, mbuf in enumerate(mbufs)]
    for copy in moves_in:
        copy.start()
    out_ref[...] = jnp.zeros_like(out_ref)

    def tile(i, carry):
        slot = lax.rem(i, 2)

        @pl.when(i + 1 < steps)
        def _():
            for copy in fetch(i + 1, 1 - slot):
                copy.start()

        for copy in fetch(i, slot):
            copy.wait()
        dw_tile(
            lambda start, size: nbuf[slot, pl.ds(start, size), :],
            lambda start, size: abuf[slot, pl.ds(start, size), :],
            w_ref,
            dz_ref,
            out_ref,
            place_ref[1],
        )
        return carry

    lax.fori_loop(0, steps, tile, 0)
    own = put(out_ref, place_ref[2], out_sems.at[merges, 0])
    own.start()
    for copy in moves_in:
        copy.wait()
    for copy in moves_out:
        copy.start()
    for copy in (own, *moves_out):
        copy.wait()


def weight_grad(width, col, vocab_col, ntiles, n_all, aux_all, w, whole, merges):
    tokens, vocab = n_all.shape[0], w.shape[1]
    anywhere = pl.BlockSpec(memory_space=pl.ANY)
    chunks = [chunk for chunk, _ in merges]
    held = ([] if whole is None else [whole]) + chunks
    place = jnp.stack([col // width, vocab_col, col] + [c for _, c in merges]).astype(i32)
    return pl.pallas_call(
        functools.partial(dw_kernel, len(merges)),
        grid_spec=pltpu.PrefetchScalarGridSpec(
            num_scalar_prefetch=2,
            grid=(1,),
            in_specs=[anywhere, anywhere, pl.BlockSpec((DIM, width), lambda s, place, nt: (0, place[0]))]
            + [anywhere] * len(held),
            out_specs=[pl.BlockSpec((DIM, width), lambda s, *_: (0, 0)), anywhere],
            scratch_shapes=[
                pltpu.VMEM((2, DW_TOK, DIM), bf16),
                pltpu.VMEM((2, DW_TOK, 128), f32),
                pltpu.VMEM((DW_TOK, width), bf16),
                pltpu.SemaphoreType.DMA((2, 2)),
                *(pltpu.VMEM(chunk.shape, f32) for chunk in chunks),
                pltpu.SemaphoreType.DMA((len(merges) + 1, 2)),
            ],
        ),
        out_shape=[
            jax.ShapeDtypeStruct((DIM, width), f32),
            jax.ShapeDtypeStruct((DIM, vocab), f32),
        ],
        input_output_aliases={} if whole is None else {5: 1},
        compiler_params=pltpu.CompilerParams(dimension_semantics=("arbitrary",)),
        cost_estimate=pl.CostEstimate(
            flops=2 * tokens * DIM * width, bytes_accessed=2 * tokens * DIM + 8 * DIM * width, transcendentals=tokens * width // 2
        ),
        name="weight_grad",
    )(place, ntiles, n_all, aux_all, w, *held)


def solution(mesh):
    dp_count, vp_count = mesh.shape["dp"], mesh.shape["vp"]
    everyone = (dp_count, vp_count)

    def local_step(hidden, targets, loss_mask, norm_scale, w_head):
        vocab = w_head.shape[1]
        dp, vp = lax.axis_index("dp"), lax.axis_index("vp")
        g = norm_scale.reshape(1, DIM)

        mask = loss_mask[0]
        idx = lax.iota(i32, BLK)
        before = jnp.sum(jnp.where(idx[None, :] < idx[:, None], mask[None, :], 0), axis=1)
        kept = jnp.sum(mask)
        pos = jnp.where(mask == 1, before, kept + idx - before)
        perm = pos[None, :] == idx[:, None]
        x_sorted = jnp.dot(perm.astype(bf16), hidden[0], preferred_element_type=f32)
        t_sorted = jnp.sum(jnp.where(perm, targets[0][None, :], 0), axis=1)
        inv_rms = lax.rsqrt(jnp.mean(x_sorted * x_sorted, axis=-1, keepdims=True) + EPS)
        x_hat = x_sorted * inv_rms

        core_pairs = [(v, v ^ 1) for v in range(vp_count)]
        x_pairs = [(v, v ^ 2) for v in range(vp_count)]
        from_core = lax.ppermute(x_hat, "vp", core_pairs)
        from_x = lax.ppermute(x_hat, "vp", x_pairs)
        xh_a = lax.all_gather(x_hat[: BLK // 2], ("dp", "vp"), axis=0, tiled=True)
        xh_b = lax.all_gather(x_hat[BLK // 2 :], ("dp", "vp"), axis=0, tiled=True)
        n_near, st_near = forward_stats(x_hat, from_core, g, w_head)
        from_x_core = lax.ppermute(from_x, "vp", core_pairs)
        n_far, st_far = forward_stats(from_x, from_x_core, g, w_head)

        info = jnp.stack([t_sorted.astype(f32), jnp.full((BLK,), kept.astype(f32))])[None]
        near = lax.all_gather(jnp.concatenate([st_near, st_far, info]), "vp", axis=0)
        stats = jnp.stack([jnp.stack([near[v, b ^ v] for b in range(vp_count)]) for v in range(vp_count)])
        row_max = jnp.max(stats[:, :, 0], axis=0)
        row_sum = jnp.sum(stats[:, :, 1] * jnp.exp(stats[:, :, 0] - row_max), axis=0)
        lse_row = row_max + jnp.log(row_sum)
        info_row = near[:, vp_count]
        lse_row = jnp.where(idx[None, :].astype(f32) < info_row[:, 1], lse_row, DROPPED)
        info_all = lax.all_gather(jnp.concatenate([lse_row[:, None], info_row], axis=1), "dp", axis=0, tiled=True)
        lse_all, t_all, kept_all = info_all[:, 0], info_all[:, 1], info_all[:, 2, 0].astype(i32)

        weight = 1.0 / jnp.sum(kept_all).astype(f32)
        live = idx[None, :] < kept_all[:, None]
        w_all = jnp.where(live, weight, 0.0)
        lse_all = jnp.where(live, lse_all * LOG2E - jnp.log2(weight), DROPPED)
        none = jnp.zeros_like(w_all)
        aux_all = jnp.stack([lse_all, w_all, t_all] + [none] * 5, axis=1)

        span = (kept_all + ALIGN - 1) // ALIGN * ALIGN
        span_a = jnp.minimum(span, BLK // 2)
        ends = jnp.cumsum(jnp.concatenate([span_a, span - span_a]))
        offs = jnp.concatenate([jnp.zeros((1,), i32), ends])
        count = dp_count * vp_count
        nt_all = ((ends[-1:] + DW_TOK - 1) // DW_TOK).astype(i32)

        first = dp * vp_count
        kept_row = lax.dynamic_slice(kept_all, (first,), (vp_count,))
        span_row = lax.dynamic_slice(span, (first,), (vp_count,))
        aux_row = lax.dynamic_slice(aux_all, (first, 0, 0), (vp_count, 8, BLK))
        offs_row = jnp.cumsum(span_row) - span_row
        nt_row = ((jnp.sum(span_row) + BLK - 1) // BLK).reshape(1)
        mine = jnp.bitwise_xor(jnp.arange(vp_count, dtype=i32), vp)
        dn_part, t_part = backward_dn(
            offs_row, span_row, kept_row, mine, nt_row, (vp * vocab).reshape(1), n_near, n_far, aux_row, w_head
        )
        d_normed = lax.psum_scatter(dn_part, "vp", scatter_dimension=0, tiled=True)

        d_scale = jnp.sum(d_normed * x_hat, axis=0)
        e = d_normed * norm_scale
        d_x = inv_rms * (e - x_hat * jnp.mean(e * x_hat, axis=-1, keepdims=True))
        back = perm.astype(bf16).T
        d_x = jnp.dot(back, d_x.astype(bf16), preferred_element_type=f32).astype(bf16)
        lse_own = lax.dynamic_slice(lse_row, (vp, 0), (1, BLK))[0]
        loss_part = weight * jnp.sum(jnp.where(idx < kept, lse_own, 0.0)) - jnp.sum(t_part)
        parts = jnp.concatenate([d_scale.reshape(6, 128), jnp.full((2, 128), loss_part, f32)])

        half, quarter = vocab // 2, vocab // 4
        y_pairs = [(d, d ^ 1) for d in range(dp_count)]
        z_pairs = [(d, d ^ 2) for d in range(dp_count)]

        def jobs_of(widths, base, where, pairs):
            starts = [sum(widths[:c]) for c in range(len(widths))]
            return [(n, base + where * quarter + c, base + (1 - where) * quarter + c, pairs) for n, c in zip(widths, starts)]

        y_jobs = jobs_of(Y_WIDTHS, 0, dp % 2, y_pairs)
        z_jobs = jobs_of(Z_WIDTHS, half, (dp // 2) % 2, z_pairs)
        jobs = [job for pair in zip(y_jobs, z_jobs) for job in pair] + z_jobs[len(y_jobs) :]

        width, col, other, pairs = jobs[0]
        place = jnp.stack([col // width, vp * vocab + col]).astype(i32)
        before = first_columns(0, offs[: count + 1], place, xh_a, aux_all, g, w_head, None)
        n_all, auxc_all, chunk = first_columns(1, offs[count:], place, xh_b, aux_all, g, w_head, before)
        moved = [(lax.ppermute(chunk, "dp", pairs), other)]
        whole = None
        for k, (width, col, other, pairs) in enumerate(jobs):
            if k == 0:
                own = (chunk, col)
                continue
            merges = [own] if k == 1 else [moved[k - LAG]] if k >= LAG else []
            chunk, whole = weight_grad(width, col, vp * vocab + col, nt_all, n_all, auxc_all, w_head, whole, merges)
            if k == len(jobs) - 1:
                chunk, parts = lax.optimization_barrier((chunk, parts))
            moved.append((lax.ppermute(chunk, "dp", pairs), other))
        parts = jnp.sum(tiny_gather(parts, everyone, 1), axis=0)
        for chunk, other in moved[-LAG:]:
            whole = lax.dynamic_update_slice(whole, chunk, (0, other))
        return parts[6, 0], d_x[None], whole, parts[:6].reshape(DIM)

    return jax.shard_map(
        local_step,
        mesh=mesh,
        in_specs=(P("dp", "vp", None), P("dp", "vp"), P("dp", "vp"), P(None), P(None, "vp")),
        out_specs=(P(), P("dp", "vp", None), P(None, "vp"), P(None)),
        check_vma=False,
    )
```

```python
import functools

import jax
import jax.numpy as jnp
from jax import lax
from jax.experimental import pallas as pl
from jax.experimental.pallas import tpu as pltpu
from jax.sharding import PartitionSpec as P


EPS = 1e-5
BLK = 512
DIM = 768
ALIGN = 16
FWD_COLS = 2048
FWD_GROUPS = (256, 1024)
DN_COLS = 2048
DW_TOK = 1024
DW_GROUP = 1024
SUB = 256
Y_WIDTHS = (1024, 1024, 1024, 1024)
Z_WIDTHS = (1024, 1024, 1024, 512)
OWN_WIDTHS = (1024,)
LAG = 4
DROPPED = 1e30
LOG2E = 1.4426950408889634


f32, bf16, i32 = jnp.float32, jnp.bfloat16, jnp.int32


def tiny_gather_kernel(dp_count, vp_count, x_ref, out_ref, send_sems, recv_sems):
    count = dp_count * vp_count
    me = lax.axis_index("dp") * vp_count + lax.axis_index("vp")
    barrier = pltpu.get_barrier_semaphore()

    def peer(k):
        other = lax.rem(me + k, count)
        return (other // vp_count, lax.rem(other, vp_count))

    for k in range(1, count):
        pl.semaphore_signal(barrier, inc=1, device_id=peer(k), device_id_type=pl.DeviceIdType.MESH)
    pl.semaphore_wait(barrier, count - 1)
    copies = [
        pltpu.make_async_remote_copy(
            src_ref=x_ref,
            dst_ref=out_ref.at[me],
            send_sem=send_sems.at[k - 1],
            recv_sem=recv_sems.at[k - 1],
            device_id=peer(k),
            device_id_type=pl.DeviceIdType.MESH,
        )
        for k in range(1, count)
    ]
    for copy in copies:
        copy.start()
    out_ref[me] = x_ref[...]
    for copy in copies:
        copy.wait()


def tiny_gather(x, mesh_shape, collective_id):
    dp_count, vp_count = mesh_shape
    count = dp_count * vp_count
    return pl.pallas_call(
        functools.partial(tiny_gather_kernel, dp_count, vp_count),
        out_shape=jax.ShapeDtypeStruct((count, 8, 128), f32),
        in_specs=[pl.BlockSpec(memory_space=pltpu.VMEM)],
        out_specs=pl.BlockSpec(memory_space=pltpu.VMEM),
        scratch_shapes=[pltpu.SemaphoreType.DMA((count - 1,)), pltpu.SemaphoreType.DMA((count - 1,))],
        compiler_params=pltpu.CompilerParams(collective_id=collective_id, has_side_effects=True),
        name="tiny_gather",
    )(x)


def place_masked(dst, off, span, new):
    rows = pl.ds(pl.multiple_of(off, ALIGN), BLK)
    live = lax.broadcasted_iota(i32, (BLK, 1), 0) < span
    dst[rows, :] = jnp.where(live, new, dst[rows, :].astype(f32)).astype(dst.dtype)


def aux_columns(aux):
    pad = jnp.zeros((120, aux.shape[1]), f32)
    return jnp.concatenate([aux, pad], axis=0).T


def fwd_kernel(group, xa, xb, g_ref, w_ref, n_ref, st_ref, m_ref, s_ref, za_ref, zb_ref):
    j = pl.program_id(0)
    groups = FWD_COLS // group
    bufs = (za_ref, zb_ref)

    @pl.when(j == 0)
    def _():
        m_ref[...] = jnp.full_like(m_ref, -DROPPED)
        s_ref[...] = jnp.zeros_like(s_ref)
        zb_ref[...] = jnp.full_like(zb_ref, -DROPPED)
        for k, x_ref in enumerate((xa, xb)):
            n_ref[pl.ds(k * BLK, BLK), :] = (x_ref[...] * g_ref[...]).astype(bf16)

    def absorb(row, z_ref):
        for r in range(0, BLK, 8):
            rows = pl.ds(pl.multiple_of(row + r, 8), 8)
            parts = [z_ref[r : r + 8, k * 128 : (k + 1) * 128] for k in range(group // 128)]
            m_old = m_ref[rows, :]
            m_new = jnp.maximum(functools.reduce(jnp.maximum, parts), m_old)
            total = functools.reduce(jnp.add, [jnp.exp(part - m_new) for part in parts])
            s_ref[rows, :] = s_ref[rows, :] * jnp.exp(m_old - m_new) + total
            m_ref[rows, :] = m_new

    def tile(i, carry):
        row = pl.multiple_of(i * BLK, BLK)
        n = n_ref[pl.ds(row, BLK), :]
        for c in range(groups):
            cols = pl.ds(c * group, group)
            bufs[c % 2][...] = jnp.dot(n, w_ref[:, cols], preferred_element_type=f32)
            absorb(row if c else pl.multiple_of((1 - i) * BLK, BLK), bufs[(c + 1) % 2])
        return carry

    lax.fori_loop(0, 2, tile, 0)

    @pl.when(j == pl.num_programs(0) - 1)
    def _():
        absorb(BLK, zb_ref)
        for k in range(2):
            rows = pl.ds(k * BLK, BLK)
            m_lane = m_ref[rows, :]
            m = jnp.max(m_lane, axis=1, keepdims=True)
            s = jnp.sum(s_ref[rows, :] * jnp.exp(m_lane - m), axis=1, keepdims=True)
            st_ref[k, 0:1, :] = jnp.broadcast_to(m, (BLK, 128)).T[0:1, :]
            st_ref[k, 1:2, :] = jnp.broadcast_to(s, (BLK, 128)).T[0:1, :]


def forward_stats(group, xa, xb, g, w):
    vocab = w.shape[1]
    return pl.pallas_call(
        functools.partial(fwd_kernel, group),
        grid=(vocab // FWD_COLS,),
        in_specs=[pl.BlockSpec((BLK, DIM), lambda j: (0, 0))] * 2
        + [
            pl.BlockSpec((1, DIM), lambda j: (0, 0)),
            pl.BlockSpec((DIM, FWD_COLS), lambda j: (0, j)),
        ],
        out_specs=[
            pl.BlockSpec((2 * BLK, DIM), lambda j: (0, 0)),
            pl.BlockSpec((2, 2, BLK), lambda j: (0, 0, 0)),
        ],
        scratch_shapes=[
            pltpu.VMEM((2 * BLK, 128), f32),
            pltpu.VMEM((2 * BLK, 128), f32),
            pltpu.VMEM((BLK, group), f32),
            pltpu.VMEM((BLK, group), f32),
        ],
        out_shape=[
            jax.ShapeDtypeStruct((2 * BLK, DIM), bf16),
            jax.ShapeDtypeStruct((2, 2, BLK), f32),
        ],
        compiler_params=pltpu.CompilerParams(dimension_semantics=("arbitrary",)),
        cost_estimate=pl.CostEstimate(
            flops=2 * 2 * BLK * DIM * vocab, bytes_accessed=2 * DIM * vocab + 5 * BLK * DIM * 4, transcendentals=2 * BLK * vocab
        ),
        name="fwd_stats",
    )(xa, xb, g, w)


def grad_logits(z, aux, col0):
    target = aux[:, 2:3].astype(i32) - col0
    hot = lax.broadcasted_iota(i32, z.shape, 1) == target
    p = jnp.exp2(z * LOG2E - aux[:, 0:1])
    return jnp.where(hot, p - aux[:, 1:2], p).astype(bf16), hot


def dn_kernel(
    offs_ref, span_ref, kept_ref, mine_ref, nt_ref, col_ref, na_ref, nb_ref, aux_ref, w_ref, dn_ref, tl_ref, acc_ref, auxc_ref, n_ref, dz_ref
):
    j = pl.program_id(0)

    @pl.when(j == 0)
    def _():
        acc_ref[...] = jnp.zeros_like(acc_ref)
        auxc_ref[...] = jnp.zeros_like(auxc_ref)
        tl_ref[...] = jnp.zeros_like(tl_ref)
        n_ref[...] = jnp.zeros_like(n_ref)
        for b in range(4):
            place_masked(auxc_ref, offs_ref[b], span_ref[b], aux_columns(aux_ref[b]))
            src = (na_ref, na_ref, nb_ref, nb_ref)[b][pl.ds(b % 2 * BLK, BLK), :].astype(f32)
            place_masked(n_ref, offs_ref[mine_ref[b]], span_ref[mine_ref[b]], src)

    col0 = col_ref[0] + j * DN_COLS

    def tile(i, carry):
        rows = pl.ds(pl.multiple_of(i * BLK, BLK), BLK)
        aux = auxc_ref[rows, :]
        n = n_ref[rows, :]
        found = jnp.zeros((BLK, 128), f32)
        for c in range(DN_COLS // 512):
            z = jnp.dot(n, w_ref[:, c * 512 : (c + 1) * 512], preferred_element_type=f32)
            dz, hot = grad_logits(z, aux, col0 + c * 512)
            dz_ref[:, c * 512 : (c + 1) * 512] = dz
            picked = jnp.where(hot, z, 0.0)
            for k in range(4):
                found += picked[:, k * 128 : (k + 1) * 128]
        tl_ref[...] += jnp.sum((found * aux[:, 1:2]).reshape(BLK // 8, 8, 128), axis=0)
        acc_ref[rows, :] += lax.dot_general(dz_ref[...], w_ref[...], (((1,), (1,)), ((), ())), preferred_element_type=f32)
        return carry

    lax.fori_loop(0, nt_ref[0], tile, 0)

    @pl.when(j == pl.num_programs(0) - 1)
    def _():
        for b in range(4):
            got = acc_ref[pl.ds(pl.multiple_of(offs_ref[b], ALIGN), BLK), :]
            live = lax.broadcasted_iota(i32, (BLK, 1), 0) < kept_ref[b]
            dn_ref[pl.ds(b * BLK, BLK), :] = jnp.where(live, got, 0.0)


def backward_dn(offs, span, kept, mine, ntiles, col0, n_near, n_far, aux_row, w):
    vocab = w.shape[1]
    return pl.pallas_call(
        dn_kernel,
        grid_spec=pltpu.PrefetchScalarGridSpec(
            num_scalar_prefetch=6,
            grid=(vocab // DN_COLS,),
            in_specs=[
                pl.BlockSpec((2 * BLK, DIM), lambda j, *_: (0, 0)),
                pl.BlockSpec((2 * BLK, DIM), lambda j, *_: (0, 0)),
                pl.BlockSpec((4, 8, BLK), lambda j, *_: (0, 0, 0)),
                pl.BlockSpec((DIM, DN_COLS), lambda j, *_: (0, j)),
            ],
            out_specs=[
                pl.BlockSpec((4 * BLK, DIM), lambda j, *_: (0, 0)),
                pl.BlockSpec((8, 128), lambda j, *_: (0, 0)),
            ],
            scratch_shapes=[
                pltpu.VMEM((4 * BLK, DIM), f32),
                pltpu.VMEM((4 * BLK, 128), f32),
                pltpu.VMEM((4 * BLK, DIM), bf16),
                pltpu.VMEM((BLK, DN_COLS), bf16),
            ],
        ),
        out_shape=[
            jax.ShapeDtypeStruct((4 * BLK, DIM), f32),
            jax.ShapeDtypeStruct((8, 128), f32),
        ],
        compiler_params=pltpu.CompilerParams(dimension_semantics=("arbitrary",)),
        cost_estimate=pl.CostEstimate(
            flops=4 * 4 * BLK * DIM * vocab, bytes_accessed=2 * DIM * vocab + 6 * BLK * DIM * 4, transcendentals=4 * BLK * vocab
        ),
        name="backward_dn",
    )(offs, span, kept, mine, ntiles, col0, n_near, n_far, aux_row, w)


def dw_tile(load, aux, w_ref, dz_ref, acc_ref, col0):
    width = acc_ref.shape[1]
    group = min(width, DW_GROUP)
    sub = SUB if width > 256 else 2 * SUB
    for c in range(width // group):
        cols = pl.ds(c * group, group)
        for u in range(DW_TOK // sub):
            rows = pl.ds(u * sub, sub)
            z = jnp.dot(load(u * sub, sub), w_ref[:, cols], preferred_element_type=f32)
            dz_ref[rows, cols], _ = grad_logits(z, aux(u * sub, sub), col0 + c * group)
        acc_ref[:, cols] += lax.dot_general(
            load(0, DW_TOK), dz_ref[:, cols], (((0,), (0,)), ((), ())), preferred_element_type=f32
        )


def first_kernel(offs_ref, table_ref, xh_ref, aux_ref, g_ref, w_ref, n_hbm, aux_hbm, acc_ref, n_img, aux_img, dz_ref, sems):
    step = pl.program_id(0)
    last = pl.num_programs(0) - 1
    end = offs_ref[offs_ref.shape[0] - 1]

    def copies(t):
        rows = pl.ds(pl.multiple_of(t * DW_TOK, DW_TOK), DW_TOK)
        return (
            pltpu.make_async_copy(n_img.at[rows, :], n_hbm.at[rows, :], sems.at[0]),
            pltpu.make_async_copy(aux_img.at[rows, :], aux_hbm.at[rows, :], sems.at[1]),
        )

    @pl.when(step == 0)
    def _():
        acc_ref[...] = jnp.zeros_like(acc_ref)

    for k in range(xh_ref.shape[0]):
        off = pl.multiple_of(offs_ref[step * xh_ref.shape[0] + k], ALIGN)
        n_img[pl.ds(off, BLK), :] = (xh_ref[k] * g_ref[...]).astype(bf16)
        aux_img[pl.ds(off, BLK), :] = aux_columns(aux_ref[k])

    @pl.when(step == last)
    def _():
        rows = pl.ds(pl.multiple_of(end, ALIGN), DW_TOK)
        n_img[rows, :] = jnp.zeros((DW_TOK, DIM), bf16)
        aux_img[rows, :] = jnp.zeros((DW_TOK, 128), f32)

    start = offs_ref[step * xh_ref.shape[0]] // DW_TOK
    stop = offs_ref[(step + 1) * xh_ref.shape[0]] // DW_TOK
    stop = jnp.where(step == last, (end + DW_TOK - 1) // DW_TOK, stop)

    def tile(t, carry):
        for copy in copies(t):
            copy.start()
        row = pl.multiple_of(t * DW_TOK, DW_TOK)
        dw_tile(
            lambda at, size: n_img[pl.ds(row + at, size), :],
            lambda at, size: aux_img[pl.ds(row + at, size), :],
            w_ref,
            dz_ref,
            acc_ref,
            table_ref[1],
        )
        return carry

    lax.fori_loop(start, stop, tile, 0)

    @pl.when(step == last)
    def _():
        def drain(t, carry):
            for copy in copies(t):
                copy.wait()
            return carry

        lax.fori_loop(0, stop, drain, 0)


def first_columns(offs, table, xh_all, aux_all, g, w):
    blocks = aux_all.shape[0]
    tokens = blocks * BLK
    width = Y_WIDTHS[0]
    each = 2
    anywhere = pl.BlockSpec(memory_space=pl.ANY)
    return pl.pallas_call(
        first_kernel,
        grid_spec=pltpu.PrefetchScalarGridSpec(
            num_scalar_prefetch=2,
            grid=(blocks // each,),
            in_specs=[
                pl.BlockSpec((each, BLK, DIM), lambda b, *_: (b, 0, 0)),
                pl.BlockSpec((each, 8, BLK), lambda b, *_: (b, 0, 0)),
                pl.BlockSpec((1, DIM), lambda b, *_: (0, 0)),
                pl.BlockSpec((DIM, width), lambda b, offs, table: (0, table[0])),
            ],
            out_specs=[anywhere, anywhere, pl.BlockSpec((DIM, width), lambda b, *_: (0, 0))],
            scratch_shapes=[
                pltpu.VMEM((tokens + DW_TOK, DIM), bf16),
                pltpu.VMEM((tokens + DW_TOK, 128), f32),
                pltpu.VMEM((DW_TOK, width), bf16),
                pltpu.SemaphoreType.DMA((2,)),
            ],
        ),
        out_shape=[
            jax.ShapeDtypeStruct((tokens, DIM), bf16),
            jax.ShapeDtypeStruct((tokens, 128), f32),
            jax.ShapeDtypeStruct((DIM, width), f32),
        ],
        compiler_params=pltpu.CompilerParams(dimension_semantics=("arbitrary",), vmem_limit_bytes=60 << 20),
        cost_estimate=pl.CostEstimate(
            flops=2 * tokens * DIM * width, bytes_accessed=6 * tokens * DIM, transcendentals=tokens * width // 2
        ),
        name="first_columns",
    )(offs, table, xh_all.reshape(blocks, BLK, DIM), aux_all, g, w)


def dw_kernel(job, places, table_ref, nt_ref, n_hbm, aux_hbm, w_ref, *rest):
    merges = len(places)
    inputs, rest = rest[: -(6 + merges + 1)], rest[-(6 + merges + 1) :]
    out_ref, all_hbm, nbuf, abuf, dz_ref, sems = rest[:6]
    mbufs, out_sems = rest[6:-1], rest[-1]
    steps = nt_ref[0]

    def fetch(i, slot):
        rows = pl.ds(pl.multiple_of(i * DW_TOK, DW_TOK), DW_TOK)
        return (
            pltpu.make_async_copy(n_hbm.at[rows, :], nbuf.at[slot], sems.at[slot, 0]),
            pltpu.make_async_copy(aux_hbm.at[rows, :], abuf.at[slot], sems.at[slot, 1]),
        )

    def put(ref, col, sem):
        return pltpu.make_async_copy(ref, all_hbm.at[:, pl.ds(pl.multiple_of(col, 128), ref.shape[1])], sem)

    for copy in fetch(0, 0):
        copy.start()
    moves_in = [pltpu.make_async_copy(src, mbuf, out_sems.at[k, 0]) for k, (src, mbuf) in enumerate(zip(inputs[-merges:], mbufs))]
    moves_out = [put(mbuf, table_ref[places[k]], out_sems.at[k, 1]) for k, mbuf in enumerate(mbufs)]
    for copy in moves_in:
        copy.start()
    out_ref[...] = jnp.zeros_like(out_ref)

    def tile(i, carry):
        slot = lax.rem(i, 2)

        @pl.when(i + 1 < steps)
        def _():
            for copy in fetch(i + 1, 1 - slot):
                copy.start()

        for copy in fetch(i, slot):
            copy.wait()
        dw_tile(
            lambda start, size: nbuf[slot, pl.ds(start, size), :],
            lambda start, size: abuf[slot, pl.ds(start, size), :],
            w_ref,
            dz_ref,
            out_ref,
            table_ref[4 * job + 1],
        )
        return carry

    lax.fori_loop(0, steps, tile, 0)
    own = put(out_ref, table_ref[4 * job + 2], out_sems.at[merges, 0])
    own.start()
    for copy in moves_in:
        copy.wait()
    for copy in moves_out:
        copy.start()
    for copy in (own, *moves_out):
        copy.wait()


def weight_grad(job, width, table, ntiles, n_all, aux_all, w, whole, merges):
    tokens, vocab = n_all.shape[0], w.shape[1]
    anywhere = pl.BlockSpec(memory_space=pl.ANY)
    chunks = [chunk for chunk, _ in merges]
    held = ([] if whole is None else [whole]) + chunks
    return pl.pallas_call(
        functools.partial(dw_kernel, job, [at for _, at in merges]),
        grid_spec=pltpu.PrefetchScalarGridSpec(
            num_scalar_prefetch=2,
            grid=(1,),
            in_specs=[anywhere, anywhere, pl.BlockSpec((DIM, width), lambda s, table, nt: (0, table[4 * job]))]
            + [anywhere] * len(held),
            out_specs=[pl.BlockSpec((DIM, width), lambda s, *_: (0, 0)), anywhere],
            scratch_shapes=[
                pltpu.VMEM((2, DW_TOK, DIM), bf16),
                pltpu.VMEM((2, DW_TOK, 128), f32),
                pltpu.VMEM((DW_TOK, width), bf16),
                pltpu.SemaphoreType.DMA((2, 2)),
                *(pltpu.VMEM(chunk.shape, f32) for chunk in chunks),
                pltpu.SemaphoreType.DMA((len(merges) + 1, 2)),
            ],
        ),
        out_shape=[
            jax.ShapeDtypeStruct((DIM, width), f32),
            jax.ShapeDtypeStruct((DIM, vocab), f32),
        ],
        input_output_aliases={} if whole is None else {5: 1},
        compiler_params=pltpu.CompilerParams(dimension_semantics=("arbitrary",)),
        cost_estimate=pl.CostEstimate(
            flops=2 * tokens * DIM * width, bytes_accessed=2 * tokens * DIM + 8 * DIM * width, transcendentals=tokens * width // 2
        ),
        name="weight_grad",
    )(table, ntiles, n_all, aux_all, w, *held)


def solution(mesh):
    dp_count, vp_count = mesh.shape["dp"], mesh.shape["vp"]
    everyone = (dp_count, vp_count)

    def local_step(hidden, targets, loss_mask, norm_scale, w_head):
        vocab = w_head.shape[1]
        dp, vp = lax.axis_index("dp"), lax.axis_index("vp")
        g = norm_scale.reshape(1, DIM)

        mask = loss_mask[0]
        idx = lax.iota(i32, BLK)
        before = jnp.sum(jnp.where(idx[None, :] < idx[:, None], mask[None, :], 0), axis=1)
        kept = jnp.sum(mask)
        pos = jnp.where(mask == 1, before, kept + idx - before)
        perm = pos[None, :] == idx[:, None]
        x_sorted = jnp.dot(perm.astype(bf16), hidden[0], preferred_element_type=f32)
        t_sorted = jnp.sum(jnp.where(perm, targets[0][None, :], 0), axis=1)
        inv_rms = lax.rsqrt(jnp.mean(x_sorted * x_sorted, axis=-1, keepdims=True) + EPS)
        x_hat = x_sorted * inv_rms

        core_pairs = [(v, v ^ 1) for v in range(vp_count)]
        x_pairs = [(v, v ^ 2) for v in range(vp_count)]
        from_core = lax.ppermute(x_hat, "vp", core_pairs)
        from_x = lax.ppermute(x_hat, "vp", x_pairs)
        xh_all = lax.all_gather(x_hat, ("dp", "vp"), axis=0, tiled=True)
        n_near, st_near = forward_stats(FWD_GROUPS[0], x_hat, from_core, g, w_head)
        from_x_core = lax.ppermute(from_x, "vp", core_pairs)
        n_far, st_far = forward_stats(FWD_GROUPS[1], from_x, from_x_core, g, w_head)

        info = jnp.stack([t_sorted.astype(f32), jnp.full((BLK,), kept.astype(f32))])[None]
        near = lax.all_gather(jnp.concatenate([st_near, st_far, info]), "vp", axis=0)
        stats = jnp.stack([jnp.stack([near[v, b ^ v] for b in range(vp_count)]) for v in range(vp_count)])
        row_max = jnp.max(stats[:, :, 0], axis=0)
        row_sum = jnp.sum(stats[:, :, 1] * jnp.exp(stats[:, :, 0] - row_max), axis=0)
        lse_row = row_max + jnp.log(row_sum)
        info_row = near[:, vp_count]
        lse_row = jnp.where(idx[None, :].astype(f32) < info_row[:, 1], lse_row, DROPPED)
        info_all = lax.all_gather(jnp.concatenate([lse_row[:, None], info_row], axis=1), "dp", axis=0, tiled=True)
        lse_all, t_all, kept_all = info_all[:, 0], info_all[:, 1], info_all[:, 2, 0].astype(i32)

        weight = 1.0 / jnp.sum(kept_all).astype(f32)
        live = idx[None, :] < kept_all[:, None]
        w_all = jnp.where(live, weight, 0.0)
        lse_all = jnp.where(live, lse_all * LOG2E - jnp.log2(weight), DROPPED)
        none = jnp.zeros_like(w_all)
        aux_all = jnp.stack([lse_all, w_all, t_all] + [none] * 5, axis=1)

        span = (kept_all + ALIGN - 1) // ALIGN * ALIGN
        ends = jnp.cumsum(span)
        offs = jnp.concatenate([jnp.zeros((1,), i32), ends])
        nt_all = ((ends[-1:] + DW_TOK - 1) // DW_TOK).astype(i32)

        first = dp * vp_count
        kept_row = lax.dynamic_slice(kept_all, (first,), (vp_count,))
        span_row = lax.dynamic_slice(span, (first,), (vp_count,))
        aux_row = lax.dynamic_slice(aux_all, (first, 0, 0), (vp_count, 8, BLK))
        offs_row = jnp.cumsum(span_row) - span_row
        nt_row = ((jnp.sum(span_row) + BLK - 1) // BLK).reshape(1)
        mine = jnp.bitwise_xor(jnp.arange(vp_count, dtype=i32), vp)
        dn_part, t_part = backward_dn(
            offs_row, span_row, kept_row, mine, nt_row, (vp * vocab).reshape(1), n_near, n_far, aux_row, w_head
        )
        d_normed = lax.psum_scatter(dn_part, "vp", scatter_dimension=0, tiled=True)

        d_scale = jnp.sum(d_normed * x_hat, axis=0)
        e = d_normed * norm_scale
        d_x = inv_rms * (e - x_hat * jnp.mean(e * x_hat, axis=-1, keepdims=True))
        back = perm.astype(bf16).T
        d_x = jnp.dot(back, d_x.astype(bf16), preferred_element_type=f32).astype(bf16)
        lse_own = lax.dynamic_slice(lse_row, (vp, 0), (1, BLK))[0]
        loss_part = weight * jnp.sum(jnp.where(idx < kept, lse_own, 0.0)) - jnp.sum(t_part)
        parts = jnp.concatenate([d_scale.reshape(6, 128), jnp.full((2, 128), loss_part, f32)])

        y_pairs = [(d, d ^ 1) for d in range(dp_count)]
        z_pairs = [(d, d ^ 2) for d in range(dp_count)]
        y_jobs, z_jobs, own_jobs, base = [], [], [], 0
        for widths, jobs, pairs in ((Y_WIDTHS, y_jobs, y_pairs), (Z_WIDTHS, z_jobs, z_pairs), (OWN_WIDTHS, own_jobs, None)):
            for n in dict.fromkeys(widths):
                stride = n * widths.count(n)
                jobs += [
                    (n, base + n * c, stride if pairs is y_pairs else 0, stride if pairs is z_pairs else 0, pairs)
                    for c in range(widths.count(n))
                ]
                base += stride * (2 if pairs else 1)
        jobs = [job for pair in zip(y_jobs, z_jobs) for job in pair] + own_jobs
        start, y_step, z_step, v_step = (
            jnp.array([x for job in jobs for x in entries(job)], i32)
            for entries in (
                lambda j: (j[1] // j[0], j[1], j[1], j[1] + j[2] + j[3]),
                lambda j: (j[2] // j[0], j[2], j[2], -j[2]),
                lambda j: (j[3] // j[0], j[3], j[3], -j[3]),
                lambda j: (0, vocab, 0, 0),
            )
        )
        table = start + y_step * (dp % 2) + z_step * (dp // 2 % 2) + v_step * vp

        n_all, auxc_all, chunk = first_columns(offs, table, xh_all, aux_all, g, w_head)
        own, whole, moved = (chunk, 2), None, []
        for k, (width, *_, pairs) in enumerate(jobs):
            if k:
                merges = [own] if k == 1 else [moved[k - LAG]] if k >= LAG else []
                chunk, whole = weight_grad(k, width, table, nt_all, n_all, auxc_all, w_head, whole, merges)
            if k == len(jobs) - 1:
                whole, parts = lax.optimization_barrier((whole, parts))
            if pairs:
                moved.append((lax.ppermute(chunk, "dp", pairs), 4 * k + 3))
        parts = jnp.sum(tiny_gather(parts, everyone, 1), axis=0)
        for chunk, at in moved[len(jobs) - LAG :]:
            whole = lax.dynamic_update_slice(whole, chunk, (0, table[at]))
        return parts[6, 0], d_x[None], whole, parts[:6].reshape(DIM)

    return jax.shard_map(
        local_step,
        mesh=mesh,
        in_specs=(P("dp", "vp", None), P("dp", "vp"), P("dp", "vp"), P(None), P(None, "vp")),
        out_specs=(P(), P("dp", "vp", None), P(None, "vp"), P(None)),
        check_vma=False,
    )
```

```python
import functools

import jax
import jax.numpy as jnp
from jax import lax
from jax.experimental import pallas as pl
from jax.experimental.pallas import tpu as pltpu
from jax.sharding import PartitionSpec as P


EPS = 1e-5
BLK = 512
DIM = 768
ALIGN = 16
FWD_COLS = 2048
FWD_GROUP = 1024
DN_COLS = 2048
DW_TOK = 1024
DW_GROUP = 1024
SUB = 256
Y_WIDTHS = (1024, 1024, 1024, 1024)
Z_WIDTHS = (1024, 1024, 1024, 512)
OWN_WIDTHS = (1024,)
LAG = 4
DROPPED = 1e30
LOG2E = 1.4426950408889634


f32, bf16, i32 = jnp.float32, jnp.bfloat16, jnp.int32


def tiny_gather_kernel(dp_count, vp_count, x_ref, out_ref, send_sems, recv_sems):
    count = dp_count * vp_count
    me = lax.axis_index("dp") * vp_count + lax.axis_index("vp")
    barrier = pltpu.get_barrier_semaphore()

    def peer(k):
        other = lax.rem(me + k, count)
        return (other // vp_count, lax.rem(other, vp_count))

    for k in range(1, count):
        pl.semaphore_signal(barrier, inc=1, device_id=peer(k), device_id_type=pl.DeviceIdType.MESH)
    pl.semaphore_wait(barrier, count - 1)
    copies = [
        pltpu.make_async_remote_copy(
            src_ref=x_ref,
            dst_ref=out_ref.at[me],
            send_sem=send_sems.at[k - 1],
            recv_sem=recv_sems.at[k - 1],
            device_id=peer(k),
            device_id_type=pl.DeviceIdType.MESH,
        )
        for k in range(1, count)
    ]
    for copy in copies:
        copy.start()
    out_ref[me] = x_ref[...]
    for copy in copies:
        copy.wait()


def tiny_gather(x, mesh_shape, collective_id):
    dp_count, vp_count = mesh_shape
    count = dp_count * vp_count
    return pl.pallas_call(
        functools.partial(tiny_gather_kernel, dp_count, vp_count),
        out_shape=jax.ShapeDtypeStruct((count, 8, 128), f32),
        in_specs=[pl.BlockSpec(memory_space=pltpu.VMEM)],
        out_specs=pl.BlockSpec(memory_space=pltpu.VMEM),
        scratch_shapes=[pltpu.SemaphoreType.DMA((count - 1,)), pltpu.SemaphoreType.DMA((count - 1,))],
        compiler_params=pltpu.CompilerParams(collective_id=collective_id, has_side_effects=True),
        name="tiny_gather",
    )(x)


def place_masked(dst, off, span, new):
    rows = pl.ds(pl.multiple_of(off, ALIGN), BLK)
    live = lax.broadcasted_iota(i32, (BLK, 1), 0) < span
    dst[rows, :] = jnp.where(live, new, dst[rows, :].astype(f32)).astype(dst.dtype)


def aux_columns(aux):
    pad = jnp.zeros((120, aux.shape[1]), f32)
    return jnp.concatenate([aux, pad], axis=0).T


def fwd_kernel(group, xa, xb, g_ref, w_ref, n_ref, st_ref, m_ref, s_ref, za_ref, zb_ref):
    j = pl.program_id(0)
    groups = FWD_COLS // group
    bufs = (za_ref, zb_ref)

    @pl.when(j == 0)
    def _():
        m_ref[...] = jnp.full_like(m_ref, -DROPPED)
        s_ref[...] = jnp.zeros_like(s_ref)
        zb_ref[...] = jnp.full_like(zb_ref, -DROPPED)
        for k, x_ref in enumerate((xa, xb)):
            n_ref[pl.ds(k * BLK, BLK), :] = (x_ref[...] * g_ref[...]).astype(bf16)

    def absorb(row, z_ref):
        for r in range(0, BLK, 8):
            rows = pl.ds(pl.multiple_of(row + r, 8), 8)
            parts = [z_ref[r : r + 8, k * 128 : (k + 1) * 128] for k in range(group // 128)]
            m_old = m_ref[rows, :]
            m_new = jnp.maximum(functools.reduce(jnp.maximum, parts), m_old)
            total = functools.reduce(jnp.add, [jnp.exp(part - m_new) for part in parts])
            s_ref[rows, :] = s_ref[rows, :] * jnp.exp(m_old - m_new) + total
            m_ref[rows, :] = m_new

    def tile(i, carry):
        row = pl.multiple_of(i * BLK, BLK)
        n = n_ref[pl.ds(row, BLK), :]
        for c in range(groups):
            cols = pl.ds(c * group, group)
            bufs[c % 2][...] = jnp.dot(n, w_ref[:, cols], preferred_element_type=f32)
            absorb(row if c else pl.multiple_of((1 - i) * BLK, BLK), bufs[(c + 1) % 2])
        return carry

    lax.fori_loop(0, 2, tile, 0)

    @pl.when(j == pl.num_programs(0) - 1)
    def _():
        absorb(BLK, zb_ref)
        for k in range(2):
            rows = pl.ds(k * BLK, BLK)
            m_lane = m_ref[rows, :]
            m = jnp.max(m_lane, axis=1, keepdims=True)
            s = jnp.sum(s_ref[rows, :] * jnp.exp(m_lane - m), axis=1, keepdims=True)
            st_ref[k, 0:1, :] = jnp.broadcast_to(m, (BLK, 128)).T[0:1, :]
            st_ref[k, 1:2, :] = jnp.broadcast_to(s, (BLK, 128)).T[0:1, :]


def forward_stats(group, xa, xb, g, w):
    vocab = w.shape[1]
    return pl.pallas_call(
        functools.partial(fwd_kernel, group),
        grid=(vocab // FWD_COLS,),
        in_specs=[pl.BlockSpec((BLK, DIM), lambda j: (0, 0))] * 2
        + [
            pl.BlockSpec((1, DIM), lambda j: (0, 0)),
            pl.BlockSpec((DIM, FWD_COLS), lambda j: (0, j)),
        ],
        out_specs=[
            pl.BlockSpec((2 * BLK, DIM), lambda j: (0, 0)),
            pl.BlockSpec((2, 2, BLK), lambda j: (0, 0, 0)),
        ],
        scratch_shapes=[
            pltpu.VMEM((2 * BLK, 128), f32),
            pltpu.VMEM((2 * BLK, 128), f32),
            pltpu.VMEM((BLK, group), f32),
            pltpu.VMEM((BLK, group), f32),
        ],
        out_shape=[
            jax.ShapeDtypeStruct((2 * BLK, DIM), bf16),
            jax.ShapeDtypeStruct((2, 2, BLK), f32),
        ],
        compiler_params=pltpu.CompilerParams(dimension_semantics=("arbitrary",)),
        cost_estimate=pl.CostEstimate(
            flops=2 * 2 * BLK * DIM * vocab, bytes_accessed=2 * DIM * vocab + 5 * BLK * DIM * 4, transcendentals=2 * BLK * vocab
        ),
        name="fwd_stats",
    )(xa, xb, g, w)


def grad_logits(z, aux, col0):
    target = aux[:, 2:3].astype(i32) - col0
    hot = lax.broadcasted_iota(i32, z.shape, 1) == target
    p = jnp.exp2(z * LOG2E - aux[:, 0:1])
    return jnp.where(hot, p - aux[:, 1:2], p).astype(bf16), hot


def dn_kernel(
    offs_ref, span_ref, kept_ref, mine_ref, nt_ref, col_ref, na_ref, nb_ref, aux_ref, w_ref, dn_ref, tl_ref, acc_ref, auxc_ref, n_ref, dz_ref
):
    j = pl.program_id(0)

    @pl.when(j == 0)
    def _():
        acc_ref[...] = jnp.zeros_like(acc_ref)
        auxc_ref[...] = jnp.zeros_like(auxc_ref)
        tl_ref[...] = jnp.zeros_like(tl_ref)
        n_ref[...] = jnp.zeros_like(n_ref)
        for b in range(4):
            place_masked(auxc_ref, offs_ref[b], span_ref[b], aux_columns(aux_ref[b]))
            src = (na_ref, na_ref, nb_ref, nb_ref)[b][pl.ds(b % 2 * BLK, BLK), :].astype(f32)
            place_masked(n_ref, offs_ref[mine_ref[b]], span_ref[mine_ref[b]], src)

    col0 = col_ref[0] + j * DN_COLS

    def tile(i, carry):
        rows = pl.ds(pl.multiple_of(i * BLK, BLK), BLK)
        aux = auxc_ref[rows, :]
        n = n_ref[rows, :]
        found = jnp.zeros((BLK, 128), f32)
        for c in range(DN_COLS // 512):
            z = jnp.dot(n, w_ref[:, c * 512 : (c + 1) * 512], preferred_element_type=f32)
            dz, hot = grad_logits(z, aux, col0 + c * 512)
            dz_ref[:, c * 512 : (c + 1) * 512] = dz
            picked = jnp.where(hot, z, 0.0)
            for k in range(4):
                found += picked[:, k * 128 : (k + 1) * 128]
        tl_ref[...] += jnp.sum((found * aux[:, 1:2]).reshape(BLK // 8, 8, 128), axis=0)
        acc_ref[rows, :] += lax.dot_general(dz_ref[...], w_ref[...], (((1,), (1,)), ((), ())), preferred_element_type=f32)
        return carry

    lax.fori_loop(0, nt_ref[0], tile, 0)

    @pl.when(j == pl.num_programs(0) - 1)
    def _():
        for b in range(4):
            got = acc_ref[pl.ds(pl.multiple_of(offs_ref[b], ALIGN), BLK), :]
            live = lax.broadcasted_iota(i32, (BLK, 1), 0) < kept_ref[b]
            dn_ref[pl.ds(b * BLK, BLK), :] = jnp.where(live, got, 0.0)


def backward_dn(offs, span, kept, mine, ntiles, col0, n_near, n_far, aux_row, w):
    vocab = w.shape[1]
    return pl.pallas_call(
        dn_kernel,
        grid_spec=pltpu.PrefetchScalarGridSpec(
            num_scalar_prefetch=6,
            grid=(vocab // DN_COLS,),
            in_specs=[
                pl.BlockSpec((2 * BLK, DIM), lambda j, *_: (0, 0)),
                pl.BlockSpec((2 * BLK, DIM), lambda j, *_: (0, 0)),
                pl.BlockSpec((4, 8, BLK), lambda j, *_: (0, 0, 0)),
                pl.BlockSpec((DIM, DN_COLS), lambda j, *_: (0, j)),
            ],
            out_specs=[
                pl.BlockSpec((4 * BLK, DIM), lambda j, *_: (0, 0)),
                pl.BlockSpec((8, 128), lambda j, *_: (0, 0)),
            ],
            scratch_shapes=[
                pltpu.VMEM((4 * BLK, DIM), f32),
                pltpu.VMEM((4 * BLK, 128), f32),
                pltpu.VMEM((4 * BLK, DIM), bf16),
                pltpu.VMEM((BLK, DN_COLS), bf16),
            ],
        ),
        out_shape=[
            jax.ShapeDtypeStruct((4 * BLK, DIM), f32),
            jax.ShapeDtypeStruct((8, 128), f32),
        ],
        compiler_params=pltpu.CompilerParams(dimension_semantics=("arbitrary",)),
        cost_estimate=pl.CostEstimate(
            flops=4 * 4 * BLK * DIM * vocab, bytes_accessed=2 * DIM * vocab + 6 * BLK * DIM * 4, transcendentals=4 * BLK * vocab
        ),
        name="backward_dn",
    )(offs, span, kept, mine, ntiles, col0, n_near, n_far, aux_row, w)


def dw_tile(load, aux, w_ref, dz_ref, acc_ref, col0):
    width = acc_ref.shape[1]
    group = min(width, DW_GROUP)
    sub = SUB if width > 256 else 2 * SUB
    for c in range(width // group):
        cols = pl.ds(c * group, group)
        for u in range(DW_TOK // sub):
            rows = pl.ds(u * sub, sub)
            z = jnp.dot(load(u * sub, sub), w_ref[:, cols], preferred_element_type=f32)
            dz_ref[rows, cols], _ = grad_logits(z, aux(u * sub, sub), col0 + c * group)
        acc_ref[:, cols] += lax.dot_general(
            load(0, DW_TOK), dz_ref[:, cols], (((0,), (0,)), ((), ())), preferred_element_type=f32
        )


def first_kernel(offs_ref, table_ref, xh_ref, aux_ref, g_ref, w_ref, n_hbm, aux_hbm, acc_ref, n_img, aux_img, dz_ref, sems):
    step = pl.program_id(0)
    last = pl.num_programs(0) - 1
    end = offs_ref[offs_ref.shape[0] - 1]

    def copies(t):
        rows = pl.ds(pl.multiple_of(t * DW_TOK, DW_TOK), DW_TOK)
        return (
            pltpu.make_async_copy(n_img.at[rows, :], n_hbm.at[rows, :], sems.at[0]),
            pltpu.make_async_copy(aux_img.at[rows, :], aux_hbm.at[rows, :], sems.at[1]),
        )

    @pl.when(step == 0)
    def _():
        acc_ref[...] = jnp.zeros_like(acc_ref)

    for k in range(xh_ref.shape[0]):
        off = pl.multiple_of(offs_ref[step * xh_ref.shape[0] + k], ALIGN)
        n_img[pl.ds(off, BLK), :] = (xh_ref[k] * g_ref[...]).astype(bf16)
        aux_img[pl.ds(off, BLK), :] = aux_columns(aux_ref[k])

    @pl.when(step == last)
    def _():
        rows = pl.ds(pl.multiple_of(end, ALIGN), DW_TOK)
        n_img[rows, :] = jnp.zeros((DW_TOK, DIM), bf16)
        aux_img[rows, :] = jnp.zeros((DW_TOK, 128), f32)

    start = offs_ref[step * xh_ref.shape[0]] // DW_TOK
    stop = offs_ref[(step + 1) * xh_ref.shape[0]] // DW_TOK
    stop = jnp.where(step == last, (end + DW_TOK - 1) // DW_TOK, stop)

    def tile(t, carry):
        for copy in copies(t):
            copy.start()
        row = pl.multiple_of(t * DW_TOK, DW_TOK)
        dw_tile(
            lambda at, size: n_img[pl.ds(row + at, size), :],
            lambda at, size: aux_img[pl.ds(row + at, size), :],
            w_ref,
            dz_ref,
            acc_ref,
            table_ref[1],
        )
        return carry

    lax.fori_loop(start, stop, tile, 0)

    @pl.when(step == last)
    def _():
        def drain(t, carry):
            for copy in copies(t):
                copy.wait()
            return carry

        lax.fori_loop(0, stop, drain, 0)


def first_columns(offs, table, xh_all, aux_all, g, w):
    blocks = aux_all.shape[0]
    tokens = blocks * BLK
    width = Y_WIDTHS[0]
    each = 2
    anywhere = pl.BlockSpec(memory_space=pl.ANY)
    return pl.pallas_call(
        first_kernel,
        grid_spec=pltpu.PrefetchScalarGridSpec(
            num_scalar_prefetch=2,
            grid=(blocks // each,),
            in_specs=[
                pl.BlockSpec((each, BLK, DIM), lambda b, *_: (b, 0, 0)),
                pl.BlockSpec((each, 8, BLK), lambda b, *_: (b, 0, 0)),
                pl.BlockSpec((1, DIM), lambda b, *_: (0, 0)),
                pl.BlockSpec((DIM, width), lambda b, offs, table: (0, table[0])),
            ],
            out_specs=[anywhere, anywhere, pl.BlockSpec((DIM, width), lambda b, *_: (0, 0))],
            scratch_shapes=[
                pltpu.VMEM((tokens + DW_TOK, DIM), bf16),
                pltpu.VMEM((tokens + DW_TOK, 128), f32),
                pltpu.VMEM((DW_TOK, width), bf16),
                pltpu.SemaphoreType.DMA((2,)),
            ],
        ),
        out_shape=[
            jax.ShapeDtypeStruct((tokens, DIM), bf16),
            jax.ShapeDtypeStruct((tokens, 128), f32),
            jax.ShapeDtypeStruct((DIM, width), f32),
        ],
        compiler_params=pltpu.CompilerParams(dimension_semantics=("arbitrary",), vmem_limit_bytes=60 << 20),
        cost_estimate=pl.CostEstimate(
            flops=2 * tokens * DIM * width, bytes_accessed=6 * tokens * DIM, transcendentals=tokens * width // 2
        ),
        name="first_columns",
    )(offs, table, xh_all.reshape(blocks, BLK, DIM), aux_all, g, w)


def dw_kernel(job, places, table_ref, nt_ref, n_hbm, aux_hbm, w_ref, *rest):
    merges = len(places)
    inputs, rest = rest[: -(6 + merges + 1)], rest[-(6 + merges + 1) :]
    out_ref, all_hbm, nbuf, abuf, dz_ref, sems = rest[:6]
    mbufs, out_sems = rest[6:-1], rest[-1]
    steps = nt_ref[0]

    def fetch(i, slot):
        rows = pl.ds(pl.multiple_of(i * DW_TOK, DW_TOK), DW_TOK)
        return (
            pltpu.make_async_copy(n_hbm.at[rows, :], nbuf.at[slot], sems.at[slot, 0]),
            pltpu.make_async_copy(aux_hbm.at[rows, :], abuf.at[slot], sems.at[slot, 1]),
        )

    def put(ref, col, sem):
        return pltpu.make_async_copy(ref, all_hbm.at[:, pl.ds(pl.multiple_of(col, 128), ref.shape[1])], sem)

    for copy in fetch(0, 0):
        copy.start()
    moves_in = [pltpu.make_async_copy(src, mbuf, out_sems.at[k, 0]) for k, (src, mbuf) in enumerate(zip(inputs[-merges:], mbufs))]
    moves_out = [put(mbuf, table_ref[places[k]], out_sems.at[k, 1]) for k, mbuf in enumerate(mbufs)]
    for copy in moves_in:
        copy.start()
    out_ref[...] = jnp.zeros_like(out_ref)

    def tile(i, carry):
        slot = lax.rem(i, 2)

        @pl.when(i + 1 < steps)
        def _():
            for copy in fetch(i + 1, 1 - slot):
                copy.start()

        for copy in fetch(i, slot):
            copy.wait()
        dw_tile(
            lambda start, size: nbuf[slot, pl.ds(start, size), :],
            lambda start, size: abuf[slot, pl.ds(start, size), :],
            w_ref,
            dz_ref,
            out_ref,
            table_ref[4 * job + 1],
        )
        return carry

    lax.fori_loop(0, steps, tile, 0)
    own = put(out_ref, table_ref[4 * job + 2], out_sems.at[merges, 0])
    own.start()
    for copy in moves_in:
        copy.wait()
    for copy in moves_out:
        copy.start()
    for copy in (own, *moves_out):
        copy.wait()


def weight_grad(job, width, table, ntiles, n_all, aux_all, w, whole, merges):
    tokens, vocab = n_all.shape[0], w.shape[1]
    anywhere = pl.BlockSpec(memory_space=pl.ANY)
    chunks = [chunk for chunk, _ in merges]
    held = ([] if whole is None else [whole]) + chunks
    return pl.pallas_call(
        functools.partial(dw_kernel, job, [at for _, at in merges]),
        grid_spec=pltpu.PrefetchScalarGridSpec(
            num_scalar_prefetch=2,
            grid=(1,),
            in_specs=[anywhere, anywhere, pl.BlockSpec((DIM, width), lambda s, table, nt: (0, table[4 * job]))]
            + [anywhere] * len(held),
            out_specs=[pl.BlockSpec((DIM, width), lambda s, *_: (0, 0)), anywhere],
            scratch_shapes=[
                pltpu.VMEM((2, DW_TOK, DIM), bf16),
                pltpu.VMEM((2, DW_TOK, 128), f32),
                pltpu.VMEM((DW_TOK, width), bf16),
                pltpu.SemaphoreType.DMA((2, 2)),
                *(pltpu.VMEM(chunk.shape, f32) for chunk in chunks),
                pltpu.SemaphoreType.DMA((len(merges) + 1, 2)),
            ],
        ),
        out_shape=[
            jax.ShapeDtypeStruct((DIM, width), f32),
            jax.ShapeDtypeStruct((DIM, vocab), f32),
        ],
        input_output_aliases={} if whole is None else {5: 1},
        compiler_params=pltpu.CompilerParams(dimension_semantics=("arbitrary",)),
        cost_estimate=pl.CostEstimate(
            flops=2 * tokens * DIM * width, bytes_accessed=2 * tokens * DIM + 8 * DIM * width, transcendentals=tokens * width // 2
        ),
        name="weight_grad",
    )(table, ntiles, n_all, aux_all, w, *held)


def finish_kernel(places, table_ref, whole_hbm, *rest):
    count = len(places)
    chunks, out_hbm, bufs, sems = rest[:count], rest[count], rest[count + 1 : -1], rest[-1]
    moves_in = [pltpu.make_async_copy(chunk, buf, sems.at[k, 0]) for k, (chunk, buf) in enumerate(zip(chunks, bufs))]
    for copy in moves_in:
        copy.start()
    moves_out = []
    for k, (at, buf) in enumerate(zip(places, bufs)):
        cols = pl.ds(pl.multiple_of(table_ref[at], 128), buf.shape[1])
        moves_out.append(pltpu.make_async_copy(buf, out_hbm.at[:, cols], sems.at[k, 1]))
        moves_in[k].wait()
        moves_out[k].start()
    for copy in moves_out:
        copy.wait()


def finish(table, whole, chunks):
    anywhere = pl.BlockSpec(memory_space=pl.ANY)
    arrays = [chunk for chunk, _ in chunks]
    return pl.pallas_call(
        functools.partial(finish_kernel, [at for _, at in chunks]),
        grid_spec=pltpu.PrefetchScalarGridSpec(
            num_scalar_prefetch=1,
            grid=(1,),
            in_specs=[anywhere] * (len(chunks) + 1),
            out_specs=anywhere,
            scratch_shapes=[pltpu.VMEM(a.shape, f32) for a in arrays] + [pltpu.SemaphoreType.DMA((len(chunks), 2))],
        ),
        out_shape=jax.ShapeDtypeStruct(whole.shape, f32),
        input_output_aliases={1: 0},
        cost_estimate=pl.CostEstimate(flops=0, bytes_accessed=sum(8 * a.size for a in arrays), transcendentals=0),
        name="finish",
    )(table, whole, *arrays)


def solution(mesh):
    dp_count, vp_count = mesh.shape["dp"], mesh.shape["vp"]
    everyone = (dp_count, vp_count)

    def local_step(hidden, targets, loss_mask, norm_scale, w_head):
        vocab = w_head.shape[1]
        dp, vp = lax.axis_index("dp"), lax.axis_index("vp")
        g = norm_scale.reshape(1, DIM)

        mask = loss_mask[0]
        idx = lax.iota(i32, BLK)
        before = jnp.sum(jnp.where(idx[None, :] < idx[:, None], mask[None, :], 0), axis=1)
        kept = jnp.sum(mask)
        pos = jnp.where(mask == 1, before, kept + idx - before)
        perm = pos[None, :] == idx[:, None]
        x_sorted = jnp.dot(perm.astype(bf16), hidden[0], preferred_element_type=f32)
        t_sorted = jnp.sum(jnp.where(perm, targets[0][None, :], 0), axis=1)
        inv_rms = lax.rsqrt(jnp.mean(x_sorted * x_sorted, axis=-1, keepdims=True) + EPS)
        x_hat = x_sorted * inv_rms

        core_pairs = [(v, v ^ 1) for v in range(vp_count)]
        x_pairs = [(v, v ^ 2) for v in range(vp_count)]
        from_core = lax.ppermute(x_hat, "vp", core_pairs)
        from_x = lax.ppermute(x_hat, "vp", x_pairs)
        xh_all = lax.all_gather(x_hat, ("dp", "vp"), axis=0, tiled=True)
        n_near, st_near = forward_stats(FWD_GROUP, x_hat, from_core, g, w_head)
        from_x_core = lax.ppermute(from_x, "vp", core_pairs)
        n_far, st_far = forward_stats(FWD_GROUP, from_x, from_x_core, g, w_head)

        info = jnp.stack([t_sorted.astype(f32), jnp.full((BLK,), kept.astype(f32))])[None]
        near = lax.all_gather(jnp.concatenate([st_near, st_far, info]), "vp", axis=0)
        stats = jnp.stack([jnp.stack([near[v, b ^ v] for b in range(vp_count)]) for v in range(vp_count)])
        row_max = jnp.max(stats[:, :, 0], axis=0)
        row_sum = jnp.sum(stats[:, :, 1] * jnp.exp(stats[:, :, 0] - row_max), axis=0)
        lse_row = row_max + jnp.log(row_sum)
        info_row = near[:, vp_count]
        lse_row = jnp.where(idx[None, :].astype(f32) < info_row[:, 1], lse_row, DROPPED)
        info_all = lax.all_gather(jnp.concatenate([lse_row[:, None], info_row], axis=1), "dp", axis=0, tiled=True)
        lse_all, t_all, kept_all = info_all[:, 0], info_all[:, 1], info_all[:, 2, 0].astype(i32)

        weight = 1.0 / jnp.sum(kept_all).astype(f32)
        live = idx[None, :] < kept_all[:, None]
        w_all = jnp.where(live, weight, 0.0)
        lse_all = jnp.where(live, lse_all * LOG2E - jnp.log2(weight), DROPPED)
        none = jnp.zeros_like(w_all)
        aux_all = jnp.stack([lse_all, w_all, t_all] + [none] * 5, axis=1)

        span = (kept_all + ALIGN - 1) // ALIGN * ALIGN
        blocks = dp_count * vp_count
        before = lax.iota(i32, blocks)[None, :] < lax.iota(i32, blocks + 1)[:, None]
        offs = jnp.sum(jnp.where(before, span[None, :], 0), axis=1)
        nt_all = (offs[blocks:] + DW_TOK - 1) // DW_TOK

        first = dp * vp_count
        kept_row = lax.dynamic_slice(kept_all, (first,), (vp_count,))
        span_row = lax.dynamic_slice(span, (first,), (vp_count,))
        aux_row = lax.dynamic_slice(aux_all, (first, 0, 0), (vp_count, 8, BLK))
        offs_row = lax.dynamic_slice(offs, (first,), (vp_count,)) - lax.dynamic_slice(offs, (first,), (1,))
        nt_row = ((jnp.sum(span_row) + BLK - 1) // BLK).reshape(1)
        mine = jnp.bitwise_xor(jnp.arange(vp_count, dtype=i32), vp)
        y_pairs = [(d, d ^ 1) for d in range(dp_count)]
        z_pairs = [(d, d ^ 2) for d in range(dp_count)]
        y_jobs, z_jobs, own_jobs, base = [], [], [], 0
        for widths, jobs, pairs in ((Y_WIDTHS, y_jobs, y_pairs), (Z_WIDTHS, z_jobs, z_pairs), (OWN_WIDTHS, own_jobs, None)):
            for n in dict.fromkeys(widths):
                stride = n * widths.count(n)
                jobs += [
                    (n, base + n * c, stride if pairs is y_pairs else 0, stride if pairs is z_pairs else 0, pairs)
                    for c in range(widths.count(n))
                ]
                base += stride * (2 if pairs else 1)
        jobs = [job for pair in zip(y_jobs, z_jobs) for job in pair] + own_jobs
        start, y_step, z_step, v_step = (
            jnp.array([x for job in jobs for x in entries(job)], i32)
            for entries in (
                lambda j: (j[1] // j[0], j[1], j[1], j[1] + j[2] + j[3]),
                lambda j: (j[2] // j[0], j[2], j[2], -j[2]),
                lambda j: (j[3] // j[0], j[3], j[3], -j[3]),
                lambda j: (0, vocab, 0, 0),
            )
        )
        table = start + y_step * (dp % 2) + z_step * (dp // 2 % 2) + v_step * vp
        aux_row, offs, nt_all, table, aux_all = lax.optimization_barrier((aux_row, offs, nt_all, table, aux_all))

        dn_part, t_part = backward_dn(
            offs_row, span_row, kept_row, mine, nt_row, (vp * vocab).reshape(1), n_near, n_far, aux_row, w_head
        )
        d_normed = lax.psum_scatter(dn_part, "vp", scatter_dimension=0, tiled=True)

        d_scale = jnp.sum(d_normed * x_hat, axis=0)
        e = d_normed * norm_scale
        d_x = inv_rms * (e - x_hat * jnp.mean(e * x_hat, axis=-1, keepdims=True))
        back = perm.astype(bf16).T
        d_x = jnp.dot(back, d_x.astype(bf16), preferred_element_type=f32).astype(bf16)
        lse_own = lax.dynamic_slice(lse_row, (vp, 0), (1, BLK))[0]
        loss_part = weight * jnp.sum(jnp.where(idx < kept, lse_own, 0.0)) - jnp.sum(t_part)
        parts = jnp.concatenate([d_scale.reshape(6, 128), jnp.full((2, 128), loss_part, f32)])

        n_all, auxc_all, chunk = first_columns(offs, table, xh_all, aux_all, g, w_head)
        own, whole, moved = (chunk, 2), None, []
        for k, (width, *_, pairs) in enumerate(jobs):
            if k:
                merges = [own] if k == 1 else [moved[k - LAG]] if k >= LAG else []
                if k == len(jobs) - 1:
                    merges.append(moved[k - LAG + 1])
                chunk, whole = weight_grad(k, width, table, nt_all, n_all, auxc_all, w_head, whole, merges)
            if k == len(jobs) - 1:
                whole, parts = lax.optimization_barrier((whole, parts))
            if pairs:
                moved.append((lax.ppermute(chunk, "dp", pairs), 4 * k + 3))
        parts = jnp.sum(tiny_gather(parts, everyone, 1), axis=0)
        whole = finish(table, whole, moved[len(jobs) - LAG + 1 :])
        return parts[6, 0], d_x[None], whole, parts[:6].reshape(DIM)

    return jax.shard_map(
        local_step,
        mesh=mesh,
        in_specs=(P("dp", "vp", None), P("dp", "vp"), P("dp", "vp"), P(None), P(None, "vp")),
        out_specs=(P(), P("dp", "vp", None), P(None, "vp"), P(None)),
        check_vma=False,
    )
```

```python
import functools

import jax
import jax.numpy as jnp
from jax import lax
from jax.experimental import pallas as pl
from jax.experimental.pallas import tpu as pltpu
from jax.sharding import PartitionSpec as P


EPS = 1e-5
BLK = 512
DIM = 768
ALIGN = 16
FWD_COLS = 2048
FWD_GROUP = 1024
DN_COLS = 2048
DW_TOK = 1024
DW_GROUP = 1024
SUB = 256
Y_WIDTHS = (1024, 1024, 1024, 1024)
Z_WIDTHS = (1024, 1024, 1024, 512)
OWN_WIDTHS = (1024,)
LAG = 4
DROPPED = 1e30
LOG2E = 1.4426950408889634


f32, bf16, i32 = jnp.float32, jnp.bfloat16, jnp.int32


def place_masked(dst, off, span, new):
    rows = pl.ds(pl.multiple_of(off, ALIGN), BLK)
    live = lax.broadcasted_iota(i32, (BLK, 1), 0) < span
    dst[rows, :] = jnp.where(live, new, dst[rows, :].astype(f32)).astype(dst.dtype)


def aux_columns(aux):
    pad = jnp.zeros((120, aux.shape[1]), f32)
    return jnp.concatenate([aux, pad], axis=0).T


def fwd_kernel(group, xa, xb, g_ref, w_ref, n_ref, st_ref, m_ref, s_ref, za_ref, zb_ref):
    j = pl.program_id(0)
    groups = FWD_COLS // group
    bufs = (za_ref, zb_ref)

    @pl.when(j == 0)
    def _():
        m_ref[...] = jnp.full_like(m_ref, -DROPPED)
        s_ref[...] = jnp.zeros_like(s_ref)
        zb_ref[...] = jnp.full_like(zb_ref, -DROPPED)
        for k, x_ref in enumerate((xa, xb)):
            n_ref[pl.ds(k * BLK, BLK), :] = (x_ref[...] * g_ref[...]).astype(bf16)

    def absorb(row, z_ref):
        for r in range(0, BLK, 8):
            rows = pl.ds(pl.multiple_of(row + r, 8), 8)
            parts = [z_ref[r : r + 8, k * 128 : (k + 1) * 128] for k in range(group // 128)]
            m_old = m_ref[rows, :]
            m_new = jnp.maximum(functools.reduce(jnp.maximum, parts), m_old)
            total = functools.reduce(jnp.add, [jnp.exp(part - m_new) for part in parts])
            s_ref[rows, :] = s_ref[rows, :] * jnp.exp(m_old - m_new) + total
            m_ref[rows, :] = m_new

    def tile(i, carry):
        row = pl.multiple_of(i * BLK, BLK)
        n = n_ref[pl.ds(row, BLK), :]
        for c in range(groups):
            cols = pl.ds(c * group, group)
            bufs[c % 2][...] = jnp.dot(n, w_ref[:, cols], preferred_element_type=f32)
            absorb(row if c else pl.multiple_of((1 - i) * BLK, BLK), bufs[(c + 1) % 2])
        return carry

    lax.fori_loop(0, 2, tile, 0)

    @pl.when(j == pl.num_programs(0) - 1)
    def _():
        absorb(BLK, zb_ref)
        for k in range(2):
            rows = pl.ds(k * BLK, BLK)
            m_lane = m_ref[rows, :]
            m = jnp.max(m_lane, axis=1, keepdims=True)
            s = jnp.sum(s_ref[rows, :] * jnp.exp(m_lane - m), axis=1, keepdims=True)
            st_ref[k, 0:1, :] = jnp.broadcast_to(m, (BLK, 128)).T[0:1, :]
            st_ref[k, 1:2, :] = jnp.broadcast_to(s, (BLK, 128)).T[0:1, :]


def forward_stats(group, xa, xb, g, w):
    vocab = w.shape[1]
    return pl.pallas_call(
        functools.partial(fwd_kernel, group),
        grid=(vocab // FWD_COLS,),
        in_specs=[pl.BlockSpec((BLK, DIM), lambda j: (0, 0))] * 2
        + [
            pl.BlockSpec((1, DIM), lambda j: (0, 0)),
            pl.BlockSpec((DIM, FWD_COLS), lambda j: (0, j)),
        ],
        out_specs=[
            pl.BlockSpec((2 * BLK, DIM), lambda j: (0, 0)),
            pl.BlockSpec((2, 2, BLK), lambda j: (0, 0, 0)),
        ],
        scratch_shapes=[
            pltpu.VMEM((2 * BLK, 128), f32),
            pltpu.VMEM((2 * BLK, 128), f32),
            pltpu.VMEM((BLK, group), f32),
            pltpu.VMEM((BLK, group), f32),
        ],
        out_shape=[
            jax.ShapeDtypeStruct((2 * BLK, DIM), bf16),
            jax.ShapeDtypeStruct((2, 2, BLK), f32),
        ],
        compiler_params=pltpu.CompilerParams(dimension_semantics=("arbitrary",)),
        cost_estimate=pl.CostEstimate(
            flops=2 * 2 * BLK * DIM * vocab, bytes_accessed=2 * DIM * vocab + 5 * BLK * DIM * 4, transcendentals=2 * BLK * vocab
        ),
        name="fwd_stats",
    )(xa, xb, g, w)


def grad_logits(z, aux, col0):
    target = aux[:, 2:3].astype(i32) - col0
    hot = lax.broadcasted_iota(i32, z.shape, 1) == target
    p = jnp.exp2(z * LOG2E - aux[:, 0:1])
    return jnp.where(hot, p - aux[:, 1:2], p).astype(bf16), hot


def dn_kernel(
    offs_ref, span_ref, kept_ref, mine_ref, nt_ref, col_ref, na_ref, nb_ref, aux_ref, w_ref, dn_ref, tl_ref, acc_ref, auxc_ref, n_ref, dz_ref
):
    j = pl.program_id(0)

    @pl.when(j == 0)
    def _():
        acc_ref[...] = jnp.zeros_like(acc_ref)
        auxc_ref[...] = jnp.zeros_like(auxc_ref)
        tl_ref[...] = jnp.zeros_like(tl_ref)
        n_ref[...] = jnp.zeros_like(n_ref)
        for b in range(4):
            place_masked(auxc_ref, offs_ref[b], span_ref[b], aux_columns(aux_ref[b]))
            src = (na_ref, na_ref, nb_ref, nb_ref)[b][pl.ds(b % 2 * BLK, BLK), :].astype(f32)
            place_masked(n_ref, offs_ref[mine_ref[b]], span_ref[mine_ref[b]], src)

    col0 = col_ref[0] + j * DN_COLS

    def tile(i, carry):
        rows = pl.ds(pl.multiple_of(i * BLK, BLK), BLK)
        aux = auxc_ref[rows, :]
        n = n_ref[rows, :]
        found = jnp.zeros((BLK, 128), f32)
        for c in range(DN_COLS // 512):
            z = jnp.dot(n, w_ref[:, c * 512 : (c + 1) * 512], preferred_element_type=f32)
            dz, hot = grad_logits(z, aux, col0 + c * 512)
            dz_ref[:, c * 512 : (c + 1) * 512] = dz
            picked = jnp.where(hot, z, 0.0)
            for k in range(4):
                found += picked[:, k * 128 : (k + 1) * 128]
        tl_ref[...] += jnp.sum((found * aux[:, 1:2]).reshape(BLK // 8, 8, 128), axis=0)
        acc_ref[rows, :] += lax.dot_general(dz_ref[...], w_ref[...], (((1,), (1,)), ((), ())), preferred_element_type=f32)
        return carry

    lax.fori_loop(0, nt_ref[0], tile, 0)

    @pl.when(j == pl.num_programs(0) - 1)
    def _():
        for b in range(4):
            got = acc_ref[pl.ds(pl.multiple_of(offs_ref[b], ALIGN), BLK), :]
            live = lax.broadcasted_iota(i32, (BLK, 1), 0) < kept_ref[b]
            dn_ref[pl.ds(b * BLK, BLK), :] = jnp.where(live, got, 0.0)


def backward_dn(offs, span, kept, mine, ntiles, col0, n_near, n_far, aux_row, w):
    vocab = w.shape[1]
    return pl.pallas_call(
        dn_kernel,
        grid_spec=pltpu.PrefetchScalarGridSpec(
            num_scalar_prefetch=6,
            grid=(vocab // DN_COLS,),
            in_specs=[
                pl.BlockSpec((2 * BLK, DIM), lambda j, *_: (0, 0)),
                pl.BlockSpec((2 * BLK, DIM), lambda j, *_: (0, 0)),
                pl.BlockSpec((4, 8, BLK), lambda j, *_: (0, 0, 0)),
                pl.BlockSpec((DIM, DN_COLS), lambda j, *_: (0, j)),
            ],
            out_specs=[
                pl.BlockSpec((4 * BLK, DIM), lambda j, *_: (0, 0)),
                pl.BlockSpec((8, 128), lambda j, *_: (0, 0)),
            ],
            scratch_shapes=[
                pltpu.VMEM((4 * BLK, DIM), f32),
                pltpu.VMEM((4 * BLK, 128), f32),
                pltpu.VMEM((4 * BLK, DIM), bf16),
                pltpu.VMEM((BLK, DN_COLS), bf16),
            ],
        ),
        out_shape=[
            jax.ShapeDtypeStruct((4 * BLK, DIM), f32),
            jax.ShapeDtypeStruct((8, 128), f32),
        ],
        compiler_params=pltpu.CompilerParams(dimension_semantics=("arbitrary",)),
        cost_estimate=pl.CostEstimate(
            flops=4 * 4 * BLK * DIM * vocab, bytes_accessed=2 * DIM * vocab + 6 * BLK * DIM * 4, transcendentals=4 * BLK * vocab
        ),
        name="backward_dn",
    )(offs, span, kept, mine, ntiles, col0, n_near, n_far, aux_row, w)


def dw_tile(tok, load, aux, w_ref, dz_ref, acc_ref, col0):
    width = acc_ref.shape[1]
    group = min(width, DW_GROUP)
    sub = SUB if width > 256 else 2 * SUB
    for c in range(width // group):
        cols = pl.ds(c * group, group)
        for u in range(tok // sub):
            rows = pl.ds(u * sub, sub)
            z = jnp.dot(load(u * sub, sub), w_ref[:, cols], preferred_element_type=f32)
            dz_ref[rows, cols], _ = grad_logits(z, aux(u * sub, sub), col0 + c * group)
        acc_ref[:, cols] += lax.dot_general(
            load(0, tok), dz_ref[pl.ds(0, tok), cols], (((0,), (0,)), ((), ())), preferred_element_type=f32
        )


def whole_tiles(count):
    halves = (count + DW_TOK // 2 - 1) // (DW_TOK // 2)
    return halves // 2, lax.rem(halves, 2)


def first_kernel(offs_ref, table_ref, xh_ref, aux_ref, g_ref, w_ref, n_hbm, aux_hbm, acc_ref, n_img, aux_img, dz_ref, sems):
    step = pl.program_id(0)
    last = pl.num_programs(0) - 1
    end = offs_ref[offs_ref.shape[0] - 1]

    def copies(t):
        rows = pl.ds(pl.multiple_of(t * DW_TOK, DW_TOK), DW_TOK)
        return (
            pltpu.make_async_copy(n_img.at[rows, :], n_hbm.at[rows, :], sems.at[0]),
            pltpu.make_async_copy(aux_img.at[rows, :], aux_hbm.at[rows, :], sems.at[1]),
        )

    @pl.when(step == 0)
    def _():
        acc_ref[...] = jnp.zeros_like(acc_ref)

    for k in range(xh_ref.shape[0]):
        off = pl.multiple_of(offs_ref[step * xh_ref.shape[0] + k], ALIGN)
        n_img[pl.ds(off, BLK), :] = (xh_ref[k] * g_ref[...]).astype(bf16)
        aux_img[pl.ds(off, BLK), :] = aux_columns(aux_ref[k])

    @pl.when(step == last)
    def _():
        rows = pl.ds(pl.multiple_of(end, ALIGN), DW_TOK)
        n_img[rows, :] = jnp.zeros((DW_TOK, DIM), bf16)
        aux_img[rows, :] = jnp.zeros((DW_TOK, 128), f32)

    start = offs_ref[step * xh_ref.shape[0]] // DW_TOK
    stop = offs_ref[(step + 1) * xh_ref.shape[0]] // DW_TOK
    full, half = whole_tiles(end)
    stop = jnp.where(step == last, full, stop)

    def add(t, tok):
        for copy in copies(t):
            copy.start()
        row = pl.multiple_of(t * DW_TOK, DW_TOK)
        dw_tile(
            tok,
            lambda at, size: n_img[pl.ds(row + at, size), :],
            lambda at, size: aux_img[pl.ds(row + at, size), :],
            w_ref,
            dz_ref,
            acc_ref,
            table_ref[1],
        )

    def tile(t, carry):
        add(t, DW_TOK)
        return carry

    lax.fori_loop(start, stop, tile, 0)

    @pl.when((step == last) & (half == 1))
    def _():
        add(full, DW_TOK // 2)

    @pl.when(step == last)
    def _():
        def drain(t, carry):
            for copy in copies(t):
                copy.wait()
            return carry

        lax.fori_loop(0, full + half, drain, 0)


def first_columns(offs, table, xh_all, aux_all, g, w):
    blocks = aux_all.shape[0]
    tokens = blocks * BLK
    width = Y_WIDTHS[0]
    each = 2
    anywhere = pl.BlockSpec(memory_space=pl.ANY)
    return pl.pallas_call(
        first_kernel,
        grid_spec=pltpu.PrefetchScalarGridSpec(
            num_scalar_prefetch=2,
            grid=(blocks // each,),
            in_specs=[
                pl.BlockSpec((each, BLK, DIM), lambda b, *_: (b, 0, 0)),
                pl.BlockSpec((each, 8, BLK), lambda b, *_: (b, 0, 0)),
                pl.BlockSpec((1, DIM), lambda b, *_: (0, 0)),
                pl.BlockSpec((DIM, width), lambda b, offs, table: (0, table[0])),
            ],
            out_specs=[anywhere, anywhere, pl.BlockSpec((DIM, width), lambda b, *_: (0, 0))],
            scratch_shapes=[
                pltpu.VMEM((tokens + DW_TOK, DIM), bf16),
                pltpu.VMEM((tokens + DW_TOK, 128), f32),
                pltpu.VMEM((DW_TOK, width), bf16),
                pltpu.SemaphoreType.DMA((2,)),
            ],
        ),
        out_shape=[
            jax.ShapeDtypeStruct((tokens, DIM), bf16),
            jax.ShapeDtypeStruct((tokens, 128), f32),
            jax.ShapeDtypeStruct((DIM, width), f32),
        ],
        compiler_params=pltpu.CompilerParams(dimension_semantics=("arbitrary",), vmem_limit_bytes=60 << 20),
        cost_estimate=pl.CostEstimate(
            flops=2 * tokens * DIM * width, bytes_accessed=6 * tokens * DIM, transcendentals=tokens * width // 2
        ),
        name="first_columns",
    )(offs, table, xh_all.reshape(blocks, BLK, DIM), aux_all, g, w)


def dw_kernel(job, places, table_ref, count_ref, n_hbm, aux_hbm, w_ref, *rest):
    merges = len(places)
    inputs, rest = rest[: -(6 + merges + 1)], rest[-(6 + merges + 1) :]
    out_ref, all_hbm, nbuf, abuf, dz_ref, sems = rest[:6]
    mbufs, out_sems = rest[6:-1], rest[-1]
    full, half = whole_tiles(count_ref[0])

    def fetch(i, slot):
        rows = pl.ds(pl.multiple_of(i * DW_TOK, DW_TOK), DW_TOK)
        return (
            pltpu.make_async_copy(n_hbm.at[rows, :], nbuf.at[slot], sems.at[slot, 0]),
            pltpu.make_async_copy(aux_hbm.at[rows, :], abuf.at[slot], sems.at[slot, 1]),
        )

    def put(ref, col, sem):
        return pltpu.make_async_copy(ref, all_hbm.at[:, pl.ds(pl.multiple_of(col, 128), ref.shape[1])], sem)

    for copy in fetch(0, 0):
        copy.start()
    moves_in = [pltpu.make_async_copy(src, mbuf, out_sems.at[k, 0]) for k, (src, mbuf) in enumerate(zip(inputs[-merges:], mbufs))]
    moves_out = [put(mbuf, table_ref[places[k]], out_sems.at[k, 1]) for k, mbuf in enumerate(mbufs)]
    for copy in moves_in:
        copy.start()
    out_ref[...] = jnp.zeros_like(out_ref)

    def add(i, tok):
        slot = lax.rem(i, 2)

        @pl.when(i + 1 < full + half)
        def _():
            for copy in fetch(i + 1, 1 - slot):
                copy.start()

        for copy in fetch(i, slot):
            copy.wait()
        dw_tile(
            tok,
            lambda start, size: nbuf[slot, pl.ds(start, size), :],
            lambda start, size: abuf[slot, pl.ds(start, size), :],
            w_ref,
            dz_ref,
            out_ref,
            table_ref[4 * job + 1],
        )

    def tile(i, carry):
        add(i, DW_TOK)
        return carry

    lax.fori_loop(0, full, tile, 0)

    @pl.when(half == 1)
    def _():
        add(full, DW_TOK // 2)

    own = put(out_ref, table_ref[4 * job + 2], out_sems.at[merges, 0])
    own.start()
    for copy in moves_in:
        copy.wait()
    for copy in moves_out:
        copy.start()
    for copy in (own, *moves_out):
        copy.wait()


def weight_grad(job, width, table, count, n_all, aux_all, w, whole, merges):
    tokens, vocab = n_all.shape[0], w.shape[1]
    anywhere = pl.BlockSpec(memory_space=pl.ANY)
    chunks = [chunk for chunk, _ in merges]
    held = ([] if whole is None else [whole]) + chunks
    return pl.pallas_call(
        functools.partial(dw_kernel, job, [at for _, at in merges]),
        grid_spec=pltpu.PrefetchScalarGridSpec(
            num_scalar_prefetch=2,
            grid=(1,),
            in_specs=[anywhere, anywhere, pl.BlockSpec((DIM, width), lambda s, table, count: (0, table[4 * job]))]
            + [anywhere] * len(held),
            out_specs=[pl.BlockSpec((DIM, width), lambda s, *_: (0, 0)), anywhere],
            scratch_shapes=[
                pltpu.VMEM((2, DW_TOK, DIM), bf16),
                pltpu.VMEM((2, DW_TOK, 128), f32),
                pltpu.VMEM((DW_TOK, width), bf16),
                pltpu.SemaphoreType.DMA((2, 2)),
                *(pltpu.VMEM(chunk.shape, f32) for chunk in chunks),
                pltpu.SemaphoreType.DMA((len(merges) + 1, 2)),
            ],
        ),
        out_shape=[
            jax.ShapeDtypeStruct((DIM, width), f32),
            jax.ShapeDtypeStruct((DIM, vocab), f32),
        ],
        input_output_aliases={} if whole is None else {5: 1},
        compiler_params=pltpu.CompilerParams(dimension_semantics=("arbitrary",)),
        cost_estimate=pl.CostEstimate(
            flops=2 * tokens * DIM * width, bytes_accessed=2 * tokens * DIM + 8 * DIM * width, transcendentals=tokens * width // 2
        ),
        name="weight_grad",
    )(table, count, n_all, aux_all, w, *held)


def finish_kernel(places, table_ref, whole_hbm, *rest):
    count = len(places)
    chunks, out_hbm, bufs, sems = rest[:count], rest[count], rest[count + 1 : -1], rest[-1]
    moves_in = [pltpu.make_async_copy(chunk, buf, sems.at[k, 0]) for k, (chunk, buf) in enumerate(zip(chunks, bufs))]
    for copy in moves_in:
        copy.start()
    moves_out = []
    for k, (at, buf) in enumerate(zip(places, bufs)):
        cols = pl.ds(pl.multiple_of(table_ref[at], 128), buf.shape[1])
        moves_out.append(pltpu.make_async_copy(buf, out_hbm.at[:, cols], sems.at[k, 1]))
        moves_in[k].wait()
        moves_out[k].start()
    for copy in moves_out:
        copy.wait()


def finish(table, whole, chunks):
    anywhere = pl.BlockSpec(memory_space=pl.ANY)
    arrays = [chunk for chunk, _ in chunks]
    return pl.pallas_call(
        functools.partial(finish_kernel, [at for _, at in chunks]),
        grid_spec=pltpu.PrefetchScalarGridSpec(
            num_scalar_prefetch=1,
            grid=(1,),
            in_specs=[anywhere] * (len(chunks) + 1),
            out_specs=anywhere,
            scratch_shapes=[pltpu.VMEM(a.shape, f32) for a in arrays] + [pltpu.SemaphoreType.DMA((len(chunks), 2))],
        ),
        out_shape=jax.ShapeDtypeStruct(whole.shape, f32),
        input_output_aliases={1: 0},
        cost_estimate=pl.CostEstimate(flops=0, bytes_accessed=sum(8 * a.size for a in arrays), transcendentals=0),
        name="finish",
    )(table, whole, *arrays)


def solution(mesh):
    dp_count, vp_count = mesh.shape["dp"], mesh.shape["vp"]

    def local_step(hidden, targets, loss_mask, norm_scale, w_head):
        vocab = w_head.shape[1]
        dp, vp = lax.axis_index("dp"), lax.axis_index("vp")
        g = norm_scale.reshape(1, DIM)

        mask = loss_mask[0]
        idx = lax.iota(i32, BLK)
        before = jnp.sum(jnp.where(idx[None, :] < idx[:, None], mask[None, :], 0), axis=1)
        kept = jnp.sum(mask)
        pos = jnp.where(mask == 1, before, kept + idx - before)
        perm = pos[None, :] == idx[:, None]
        x_sorted = jnp.dot(perm.astype(bf16), hidden[0], preferred_element_type=f32)
        t_sorted = jnp.sum(jnp.where(perm, targets[0][None, :], 0), axis=1)
        inv_rms = lax.rsqrt(jnp.mean(x_sorted * x_sorted, axis=-1, keepdims=True) + EPS)
        x_hat = x_sorted * inv_rms

        core_pairs = [(v, v ^ 1) for v in range(vp_count)]
        x_pairs = [(v, v ^ 2) for v in range(vp_count)]
        from_core = lax.ppermute(x_hat, "vp", core_pairs)
        from_x = lax.ppermute(x_hat, "vp", x_pairs)
        xh_all = lax.all_gather(x_hat, ("dp", "vp"), axis=0, tiled=True)
        n_near, st_near = forward_stats(FWD_GROUP, x_hat, from_core, g, w_head)
        from_x_core = lax.ppermute(from_x, "vp", core_pairs)
        n_far, st_far = forward_stats(FWD_GROUP, from_x, from_x_core, g, w_head)

        info = jnp.stack([t_sorted.astype(f32), jnp.full((BLK,), kept.astype(f32))])[None]
        near = lax.all_gather(jnp.concatenate([st_near, st_far, info]), "vp", axis=0)
        stats = jnp.stack([jnp.stack([near[v, b ^ v] for b in range(vp_count)]) for v in range(vp_count)])
        row_max = jnp.max(stats[:, :, 0], axis=0)
        row_sum = jnp.sum(stats[:, :, 1] * jnp.exp(stats[:, :, 0] - row_max), axis=0)
        lse_row = row_max + jnp.log(row_sum)
        info_row = near[:, vp_count]
        lse_row = jnp.where(idx[None, :].astype(f32) < info_row[:, 1], lse_row, DROPPED)
        info_all = lax.all_gather(jnp.concatenate([lse_row[:, None], info_row], axis=1), "dp", axis=0, tiled=True)
        lse_all, t_all, kept_all = info_all[:, 0], info_all[:, 1], info_all[:, 2, 0].astype(i32)

        weight = 1.0 / jnp.sum(kept_all).astype(f32)
        live = idx[None, :] < kept_all[:, None]
        w_all = jnp.where(live, weight, 0.0)
        lse_all = jnp.where(live, lse_all * LOG2E - jnp.log2(weight), DROPPED)
        none = jnp.zeros_like(w_all)
        aux_all = jnp.stack([lse_all, w_all, t_all] + [none] * 5, axis=1)

        span = (kept_all + ALIGN - 1) // ALIGN * ALIGN
        blocks = dp_count * vp_count
        before = lax.iota(i32, blocks)[None, :] < lax.iota(i32, blocks + 1)[:, None]
        offs = jnp.sum(jnp.where(before, span[None, :], 0), axis=1)
        count = offs[blocks:]

        first = dp * vp_count
        kept_row = lax.dynamic_slice(kept_all, (first,), (vp_count,))
        span_row = lax.dynamic_slice(span, (first,), (vp_count,))
        aux_row = lax.dynamic_slice(aux_all, (first, 0, 0), (vp_count, 8, BLK))
        offs_row = lax.dynamic_slice(offs, (first,), (vp_count,)) - lax.dynamic_slice(offs, (first,), (1,))
        nt_row = ((jnp.sum(span_row) + BLK - 1) // BLK).reshape(1)
        mine = jnp.bitwise_xor(jnp.arange(vp_count, dtype=i32), vp)
        y_pairs = [(d, d ^ 1) for d in range(dp_count)]
        z_pairs = [(d, d ^ 2) for d in range(dp_count)]
        y_jobs, z_jobs, own_jobs, base = [], [], [], 0
        for widths, jobs, pairs in ((Y_WIDTHS, y_jobs, y_pairs), (Z_WIDTHS, z_jobs, z_pairs), (OWN_WIDTHS, own_jobs, None)):
            for n in dict.fromkeys(widths):
                stride = n * widths.count(n)
                jobs += [
                    (n, base + n * c, stride if pairs is y_pairs else 0, stride if pairs is z_pairs else 0, pairs)
                    for c in range(widths.count(n))
                ]
                base += stride * (2 if pairs else 1)
        jobs = [job for pair in zip(y_jobs, z_jobs) for job in pair] + own_jobs
        start, y_step, z_step, v_step = (
            jnp.array([x for job in jobs for x in entries(job)], i32)
            for entries in (
                lambda j: (j[1] // j[0], j[1], j[1], j[1] + j[2] + j[3]),
                lambda j: (j[2] // j[0], j[2], j[2], -j[2]),
                lambda j: (j[3] // j[0], j[3], j[3], -j[3]),
                lambda j: (0, vocab, 0, 0),
            )
        )
        table = start + y_step * (dp % 2) + z_step * (dp // 2 % 2) + v_step * vp
        aux_row, offs, count, table, aux_all = lax.optimization_barrier((aux_row, offs, count, table, aux_all))

        dn_part, t_part = backward_dn(
            offs_row, span_row, kept_row, mine, nt_row, (vp * vocab).reshape(1), n_near, n_far, aux_row, w_head
        )
        d_normed = lax.psum_scatter(dn_part, "vp", scatter_dimension=0, tiled=True)

        d_scale = jnp.sum(d_normed * x_hat, axis=0)
        e = d_normed * norm_scale
        d_x = inv_rms * (e - x_hat * jnp.mean(e * x_hat, axis=-1, keepdims=True))
        back = perm.astype(bf16).T
        d_x = jnp.dot(back, d_x.astype(bf16), preferred_element_type=f32).astype(bf16)
        lse_own = lax.dynamic_slice(lse_row, (vp, 0), (1, BLK))[0]
        loss_part = weight * jnp.sum(jnp.where(idx < kept, lse_own, 0.0)) - jnp.sum(t_part)
        parts = jnp.concatenate([d_scale.reshape(6, 128), jnp.full((58, 128), loss_part, f32)])
        parts = lax.all_gather(parts, ("dp", "vp"), axis=0)
        parts = jnp.sum(parts[:, :8], axis=0)

        n_all, auxc_all, chunk = first_columns(offs, table, xh_all, aux_all, g, w_head)
        own, whole, moved = (chunk, 2), None, []
        for k, (width, *_, pairs) in enumerate(jobs):
            if k:
                merges = [own] if k == 1 else [moved[k - LAG]] if k >= LAG else []
                chunk, whole = weight_grad(k, width, table, count, n_all, auxc_all, w_head, whole, merges)
            if pairs:
                moved.append((lax.ppermute(chunk, "dp", pairs), 4 * k + 3))
        whole = finish(table, whole, moved[len(jobs) - LAG :])
        return parts[6, 0], d_x[None], whole, parts[:6].reshape(DIM)

    return jax.shard_map(
        local_step,
        mesh=mesh,
        in_specs=(P("dp", "vp", None), P("dp", "vp"), P("dp", "vp"), P(None), P(None, "vp")),
        out_specs=(P(), P("dp", "vp", None), P(None, "vp"), P(None)),
        check_vma=False,
    )
```

```python
import functools

import jax
import jax.numpy as jnp
from jax import lax
from jax.experimental import pallas as pl
from jax.experimental.pallas import tpu as pltpu
from jax.sharding import PartitionSpec as P


EPS = 1e-5
BLK = 512
DIM = 768
ALIGN = 16
FWD_COLS = 2048
FWD_GROUP = 1024
DN_COLS = 2048
DW_TOK = 1024
DW_GROUP = 1024
SUB = 256
Y_WIDTHS = (1024, 1024, 1024, 1024)
Z_WIDTHS = (1024, 1024, 1024, 512)
OWN_WIDTHS = (1024,)
LAG = 4
DROPPED = 1e30
LOG2E = 1.4426950408889634


f32, bf16, i32 = jnp.float32, jnp.bfloat16, jnp.int32


def place_masked(dst, off, span, new):
    rows = pl.ds(pl.multiple_of(off, ALIGN), BLK)
    live = lax.broadcasted_iota(i32, (BLK, 1), 0) < span
    dst[rows, :] = jnp.where(live, new, dst[rows, :].astype(f32)).astype(dst.dtype)


def aux_columns(aux):
    pad = jnp.zeros((120, aux.shape[1]), f32)
    return jnp.concatenate([aux, pad], axis=0).T


def fwd_kernel(group, xa, xb, g_ref, w_ref, n_ref, st_ref, m_ref, s_ref, za_ref, zb_ref):
    j = pl.program_id(0)
    groups = FWD_COLS // group
    bufs = (za_ref, zb_ref)

    @pl.when(j == 0)
    def _():
        m_ref[...] = jnp.full_like(m_ref, -DROPPED)
        s_ref[...] = jnp.zeros_like(s_ref)
        zb_ref[...] = jnp.full_like(zb_ref, -DROPPED)
        for k, x_ref in enumerate((xa, xb)):
            n_ref[pl.ds(k * BLK, BLK), :] = (x_ref[...] * g_ref[...]).astype(bf16)

    def absorb(row, z_ref):
        for r in range(0, BLK, 8):
            rows = pl.ds(pl.multiple_of(row + r, 8), 8)
            parts = [z_ref[r : r + 8, k * 128 : (k + 1) * 128] for k in range(group // 128)]
            m_old = m_ref[rows, :]
            m_new = jnp.maximum(functools.reduce(jnp.maximum, parts), m_old)
            total = functools.reduce(jnp.add, [jnp.exp(part - m_new) for part in parts])
            s_ref[rows, :] = s_ref[rows, :] * jnp.exp(m_old - m_new) + total
            m_ref[rows, :] = m_new

    def tile(i, carry):
        row = pl.multiple_of(i * BLK, BLK)
        n = n_ref[pl.ds(row, BLK), :]
        for c in range(groups):
            cols = pl.ds(c * group, group)
            bufs[c % 2][...] = jnp.dot(n, w_ref[:, cols], preferred_element_type=f32)
            absorb(row if c else pl.multiple_of((1 - i) * BLK, BLK), bufs[(c + 1) % 2])
        return carry

    lax.fori_loop(0, 2, tile, 0)

    @pl.when(j == pl.num_programs(0) - 1)
    def _():
        absorb(BLK, zb_ref)
        for k in range(2):
            rows = pl.ds(k * BLK, BLK)
            m_lane = m_ref[rows, :]
            m = jnp.max(m_lane, axis=1, keepdims=True)
            s = jnp.sum(s_ref[rows, :] * jnp.exp(m_lane - m), axis=1, keepdims=True)
            st_ref[k, 0:1, :] = jnp.broadcast_to(m, (BLK, 128)).T[0:1, :]
            st_ref[k, 1:2, :] = jnp.broadcast_to(s, (BLK, 128)).T[0:1, :]


def forward_stats(group, xa, xb, g, w):
    vocab = w.shape[1]
    return pl.pallas_call(
        functools.partial(fwd_kernel, group),
        grid=(vocab // FWD_COLS,),
        in_specs=[pl.BlockSpec((BLK, DIM), lambda j: (0, 0))] * 2
        + [
            pl.BlockSpec((1, DIM), lambda j: (0, 0)),
            pl.BlockSpec((DIM, FWD_COLS), lambda j: (0, j)),
        ],
        out_specs=[
            pl.BlockSpec((2 * BLK, DIM), lambda j: (0, 0)),
            pl.BlockSpec((2, 2, BLK), lambda j: (0, 0, 0)),
        ],
        scratch_shapes=[
            pltpu.VMEM((2 * BLK, 128), f32),
            pltpu.VMEM((2 * BLK, 128), f32),
            pltpu.VMEM((BLK, group), f32),
            pltpu.VMEM((BLK, group), f32),
        ],
        out_shape=[
            jax.ShapeDtypeStruct((2 * BLK, DIM), bf16),
            jax.ShapeDtypeStruct((2, 2, BLK), f32),
        ],
        compiler_params=pltpu.CompilerParams(dimension_semantics=("arbitrary",)),
        cost_estimate=pl.CostEstimate(
            flops=2 * 2 * BLK * DIM * vocab, bytes_accessed=2 * DIM * vocab + 5 * BLK * DIM * 4, transcendentals=2 * BLK * vocab
        ),
        name="fwd_stats",
    )(xa, xb, g, w)


def grad_logits(z, aux, col0):
    target = aux[:, 2:3].astype(i32) - col0
    hot = lax.broadcasted_iota(i32, z.shape, 1) == target
    p = jnp.exp2(z * LOG2E - aux[:, 0:1])
    return jnp.where(hot, p - aux[:, 1:2], p).astype(bf16), hot


def dn_kernel(
    offs_ref, span_ref, kept_ref, mine_ref, nt_ref, col_ref, na_ref, nb_ref, aux_ref, w_ref, dn_ref, tl_ref, acc_ref, auxc_ref, n_ref, dz_ref
):
    j = pl.program_id(0)

    @pl.when(j == 0)
    def _():
        acc_ref[...] = jnp.zeros_like(acc_ref)
        auxc_ref[...] = jnp.zeros_like(auxc_ref)
        tl_ref[...] = jnp.zeros_like(tl_ref)
        n_ref[...] = jnp.zeros_like(n_ref)
        for b in range(4):
            place_masked(auxc_ref, offs_ref[b], span_ref[b], aux_columns(aux_ref[b]))
            src = (na_ref, na_ref, nb_ref, nb_ref)[b][pl.ds(b % 2 * BLK, BLK), :].astype(f32)
            place_masked(n_ref, offs_ref[mine_ref[b]], span_ref[mine_ref[b]], src)

    col0 = col_ref[0] + j * DN_COLS

    def tile(i, carry):
        rows = pl.ds(pl.multiple_of(i * BLK, BLK), BLK)
        aux = auxc_ref[rows, :]
        n = n_ref[rows, :]
        found = jnp.zeros((BLK, 128), f32)
        for c in range(DN_COLS // 512):
            z = jnp.dot(n, w_ref[:, c * 512 : (c + 1) * 512], preferred_element_type=f32)
            dz, hot = grad_logits(z, aux, col0 + c * 512)
            dz_ref[:, c * 512 : (c + 1) * 512] = dz
            picked = jnp.where(hot, z, 0.0)
            for k in range(4):
                found += picked[:, k * 128 : (k + 1) * 128]
        tl_ref[...] += jnp.sum((found * aux[:, 1:2]).reshape(BLK // 8, 8, 128), axis=0)
        acc_ref[rows, :] += lax.dot_general(dz_ref[...], w_ref[...], (((1,), (1,)), ((), ())), preferred_element_type=f32)
        return carry

    lax.fori_loop(0, nt_ref[0], tile, 0)

    @pl.when(j == pl.num_programs(0) - 1)
    def _():
        for b in range(4):
            got = acc_ref[pl.ds(pl.multiple_of(offs_ref[b], ALIGN), BLK), :]
            live = lax.broadcasted_iota(i32, (BLK, 1), 0) < kept_ref[b]
            dn_ref[pl.ds(b * BLK, BLK), :] = jnp.where(live, got, 0.0)


def backward_dn(offs, span, kept, mine, ntiles, col0, n_near, n_far, aux_row, w):
    vocab = w.shape[1]
    return pl.pallas_call(
        dn_kernel,
        grid_spec=pltpu.PrefetchScalarGridSpec(
            num_scalar_prefetch=6,
            grid=(vocab // DN_COLS,),
            in_specs=[
                pl.BlockSpec((2 * BLK, DIM), lambda j, *_: (0, 0)),
                pl.BlockSpec((2 * BLK, DIM), lambda j, *_: (0, 0)),
                pl.BlockSpec((4, 8, BLK), lambda j, *_: (0, 0, 0)),
                pl.BlockSpec((DIM, DN_COLS), lambda j, *_: (0, j)),
            ],
            out_specs=[
                pl.BlockSpec((4 * BLK, DIM), lambda j, *_: (0, 0)),
                pl.BlockSpec((8, 128), lambda j, *_: (0, 0)),
            ],
            scratch_shapes=[
                pltpu.VMEM((4 * BLK, DIM), f32),
                pltpu.VMEM((4 * BLK, 128), f32),
                pltpu.VMEM((4 * BLK, DIM), bf16),
                pltpu.VMEM((BLK, DN_COLS), bf16),
            ],
        ),
        out_shape=[
            jax.ShapeDtypeStruct((4 * BLK, DIM), f32),
            jax.ShapeDtypeStruct((8, 128), f32),
        ],
        compiler_params=pltpu.CompilerParams(dimension_semantics=("arbitrary",)),
        cost_estimate=pl.CostEstimate(
            flops=4 * 4 * BLK * DIM * vocab, bytes_accessed=2 * DIM * vocab + 6 * BLK * DIM * 4, transcendentals=4 * BLK * vocab
        ),
        name="backward_dn",
    )(offs, span, kept, mine, ntiles, col0, n_near, n_far, aux_row, w)


def dw_tile(tok, load, aux, w_ref, dz_ref, acc_ref, col0):
    width = acc_ref.shape[1]
    group = min(width, DW_GROUP)
    sub = SUB if width > 256 else 2 * SUB
    for c in range(width // group):
        cols = pl.ds(c * group, group)
        for u in range(tok // sub):
            rows = pl.ds(u * sub, sub)
            z = jnp.dot(load(u * sub, sub), w_ref[:, cols], preferred_element_type=f32)
            dz_ref[rows, cols], _ = grad_logits(z, aux(u * sub, sub), col0 + c * group)
        acc_ref[:, cols] += lax.dot_general(
            load(0, tok), dz_ref[pl.ds(0, tok), cols], (((0,), (0,)), ((), ())), preferred_element_type=f32
        )


def whole_tiles(count):
    halves = (count + DW_TOK // 2 - 1) // (DW_TOK // 2)
    return halves // 2, lax.rem(halves, 2)


def first_kernel(offs_ref, table_ref, xh_ref, aux_ref, g_ref, w_ref, n_hbm, aux_hbm, acc_ref, n_img, aux_img, dz_ref, sems):
    step = pl.program_id(0)
    last = pl.num_programs(0) - 1
    end = offs_ref[offs_ref.shape[0] - 1]

    def copies(t):
        rows = pl.ds(pl.multiple_of(t * DW_TOK, DW_TOK), DW_TOK)
        return (
            pltpu.make_async_copy(n_img.at[rows, :], n_hbm.at[rows, :], sems.at[0]),
            pltpu.make_async_copy(aux_img.at[rows, :], aux_hbm.at[rows, :], sems.at[1]),
        )

    @pl.when(step == 0)
    def _():
        acc_ref[...] = jnp.zeros_like(acc_ref)

    for k in range(xh_ref.shape[0]):
        off = pl.multiple_of(offs_ref[step * xh_ref.shape[0] + k], ALIGN)
        n_img[pl.ds(off, BLK), :] = (xh_ref[k] * g_ref[...]).astype(bf16)
        aux_img[pl.ds(off, BLK), :] = aux_columns(aux_ref[k])

    @pl.when(step == last)
    def _():
        rows = pl.ds(pl.multiple_of(end, ALIGN), DW_TOK)
        n_img[rows, :] = jnp.zeros((DW_TOK, DIM), bf16)
        aux_img[rows, :] = jnp.zeros((DW_TOK, 128), f32)

    start = offs_ref[step * xh_ref.shape[0]] // DW_TOK
    stop = offs_ref[(step + 1) * xh_ref.shape[0]] // DW_TOK
    full, half = whole_tiles(end)
    stop = jnp.where(step == last, full, stop)

    def add(t, tok):
        for copy in copies(t):
            copy.start()
        row = pl.multiple_of(t * DW_TOK, DW_TOK)
        dw_tile(
            tok,
            lambda at, size: n_img[pl.ds(row + at, size), :],
            lambda at, size: aux_img[pl.ds(row + at, size), :],
            w_ref,
            dz_ref,
            acc_ref,
            table_ref[1],
        )

    def tile(t, carry):
        add(t, DW_TOK)
        return carry

    lax.fori_loop(start, stop, tile, 0)

    @pl.when((step == last) & (half == 1))
    def _():
        add(full, DW_TOK // 2)

    @pl.when(step == last)
    def _():
        def drain(t, carry):
            for copy in copies(t):
                copy.wait()
            return carry

        lax.fori_loop(0, full + half, drain, 0)


def first_columns(offs, table, xh_all, aux_all, g, w):
    blocks = aux_all.shape[0]
    tokens = blocks * BLK
    width = Y_WIDTHS[0]
    each = 2
    anywhere = pl.BlockSpec(memory_space=pl.ANY)
    return pl.pallas_call(
        first_kernel,
        grid_spec=pltpu.PrefetchScalarGridSpec(
            num_scalar_prefetch=2,
            grid=(blocks // each,),
            in_specs=[
                pl.BlockSpec((each, BLK, DIM), lambda b, *_: (b, 0, 0)),
                pl.BlockSpec((each, 8, BLK), lambda b, *_: (b, 0, 0)),
                pl.BlockSpec((1, DIM), lambda b, *_: (0, 0)),
                pl.BlockSpec((DIM, width), lambda b, offs, table: (0, table[0])),
            ],
            out_specs=[anywhere, anywhere, pl.BlockSpec((DIM, width), lambda b, *_: (0, 0))],
            scratch_shapes=[
                pltpu.VMEM((tokens + DW_TOK, DIM), bf16),
                pltpu.VMEM((tokens + DW_TOK, 128), f32),
                pltpu.VMEM((DW_TOK, width), bf16),
                pltpu.SemaphoreType.DMA((2,)),
            ],
        ),
        out_shape=[
            jax.ShapeDtypeStruct((tokens, DIM), bf16),
            jax.ShapeDtypeStruct((tokens, 128), f32),
            jax.ShapeDtypeStruct((DIM, width), f32),
        ],
        compiler_params=pltpu.CompilerParams(dimension_semantics=("arbitrary",), vmem_limit_bytes=60 << 20),
        cost_estimate=pl.CostEstimate(
            flops=2 * tokens * DIM * width, bytes_accessed=6 * tokens * DIM, transcendentals=tokens * width // 2
        ),
        name="first_columns",
    )(offs, table, xh_all.reshape(blocks, BLK, DIM), aux_all, g, w)


def dw_kernel(job, places, table_ref, count_ref, n_hbm, aux_hbm, w_hbm, *rest):
    merges = len(places)
    inputs, rest = rest[: -(9 + merges)], rest[-(9 + merges) :]
    chunk_hbm, all_hbm, out_ref, w_ref, nbuf, abuf, dz_ref, sems = rest[:8]
    mbufs, out_sems = rest[8:-1], rest[-1]
    full, half = whole_tiles(count_ref[0])

    def fetch(i, slot):
        rows = pl.ds(pl.multiple_of(i * DW_TOK, DW_TOK), DW_TOK)
        return (
            pltpu.make_async_copy(n_hbm.at[rows, :], nbuf.at[slot], sems.at[slot, 0]),
            pltpu.make_async_copy(aux_hbm.at[rows, :], abuf.at[slot], sems.at[slot, 1]),
        )

    def put(ref, col, sem):
        return pltpu.make_async_copy(ref, all_hbm.at[:, pl.ds(pl.multiple_of(col, 128), ref.shape[1])], sem)

    cols = pl.ds(pl.multiple_of(table_ref[4 * job + 2], 128), out_ref.shape[1])
    columns = pltpu.make_async_copy(w_hbm.at[:, cols], w_ref, out_sems.at[merges, 1])
    columns.start()
    for copy in fetch(0, 0):
        copy.start()
    moves_in = [pltpu.make_async_copy(src, mbuf, out_sems.at[k, 0]) for k, (src, mbuf) in enumerate(zip(inputs[-merges:], mbufs))]
    moves_out = [put(mbuf, table_ref[places[k]], out_sems.at[k, 1]) for k, mbuf in enumerate(mbufs)]
    for copy in moves_in:
        copy.start()
    out_ref[...] = jnp.zeros_like(out_ref)
    columns.wait()

    def add(i, tok):
        slot = lax.rem(i, 2)

        @pl.when(i + 1 < full + half)
        def _():
            for copy in fetch(i + 1, 1 - slot):
                copy.start()

        for copy in fetch(i, slot):
            copy.wait()
        dw_tile(
            tok,
            lambda start, size: nbuf[slot, pl.ds(start, size), :],
            lambda start, size: abuf[slot, pl.ds(start, size), :],
            w_ref,
            dz_ref,
            out_ref,
            table_ref[4 * job + 1],
        )

    def tile(i, carry):
        add(i, DW_TOK)
        return carry

    lax.fori_loop(0, full, tile, 0)

    @pl.when(half == 1)
    def _():
        add(full, DW_TOK // 2)

    own = put(out_ref, table_ref[4 * job + 2], out_sems.at[merges, 0])
    sent = pltpu.make_async_copy(out_ref, chunk_hbm, out_sems.at[merges, 1])
    sent.start()
    own.start()
    for copy in moves_in:
        copy.wait()
    for copy in moves_out:
        copy.start()
    for copy in (sent, own, *moves_out):
        copy.wait()


def weight_grad(job, width, table, count, n_all, aux_all, w, whole, merges):
    tokens, vocab = n_all.shape[0], w.shape[1]
    anywhere = pl.BlockSpec(memory_space=pl.ANY)
    chunks = [chunk for chunk, _ in merges]
    held = ([] if whole is None else [whole]) + chunks
    return pl.pallas_call(
        functools.partial(dw_kernel, job, [at for _, at in merges]),
        grid_spec=pltpu.PrefetchScalarGridSpec(
            num_scalar_prefetch=2,
            grid=(1,),
            in_specs=[anywhere] * (3 + len(held)),
            out_specs=[anywhere, anywhere],
            scratch_shapes=[
                pltpu.VMEM((DIM, width), f32),
                pltpu.VMEM((DIM, width), bf16),
                pltpu.VMEM((2, DW_TOK, DIM), bf16),
                pltpu.VMEM((2, DW_TOK, 128), f32),
                pltpu.VMEM((DW_TOK, width), bf16),
                pltpu.SemaphoreType.DMA((2, 2)),
                *(pltpu.VMEM(chunk.shape, f32) for chunk in chunks),
                pltpu.SemaphoreType.DMA((len(merges) + 1, 2)),
            ],
        ),
        out_shape=[
            jax.ShapeDtypeStruct((DIM, width), f32),
            jax.ShapeDtypeStruct((DIM, vocab), f32),
        ],
        input_output_aliases={} if whole is None else {5: 1},
        compiler_params=pltpu.CompilerParams(dimension_semantics=("arbitrary",)),
        cost_estimate=pl.CostEstimate(
            flops=2 * tokens * DIM * width, bytes_accessed=2 * tokens * DIM + 8 * DIM * width, transcendentals=tokens * width // 2
        ),
        name="weight_grad",
    )(table, count, n_all, aux_all, w, *held)


def finish_kernel(places, table_ref, whole_hbm, *rest):
    count = len(places)
    chunks, out_hbm, bufs, sems = rest[:count], rest[count], rest[count + 1 : -1], rest[-1]
    moves_in = [pltpu.make_async_copy(chunk, buf, sems.at[k, 0]) for k, (chunk, buf) in enumerate(zip(chunks, bufs))]
    for copy in moves_in:
        copy.start()
    moves_out = []
    for k, (at, buf) in enumerate(zip(places, bufs)):
        cols = pl.ds(pl.multiple_of(table_ref[at], 128), buf.shape[1])
        moves_out.append(pltpu.make_async_copy(buf, out_hbm.at[:, cols], sems.at[k, 1]))
        moves_in[k].wait()
        moves_out[k].start()
    for copy in moves_out:
        copy.wait()


def finish(table, whole, chunks):
    anywhere = pl.BlockSpec(memory_space=pl.ANY)
    arrays = [chunk for chunk, _ in chunks]
    return pl.pallas_call(
        functools.partial(finish_kernel, [at for _, at in chunks]),
        grid_spec=pltpu.PrefetchScalarGridSpec(
            num_scalar_prefetch=1,
            grid=(1,),
            in_specs=[anywhere] * (len(chunks) + 1),
            out_specs=anywhere,
            scratch_shapes=[pltpu.VMEM(a.shape, f32) for a in arrays] + [pltpu.SemaphoreType.DMA((len(chunks), 2))],
        ),
        out_shape=jax.ShapeDtypeStruct(whole.shape, f32),
        input_output_aliases={1: 0},
        cost_estimate=pl.CostEstimate(flops=0, bytes_accessed=sum(8 * a.size for a in arrays), transcendentals=0),
        name="finish",
    )(table, whole, *arrays)


def solution(mesh):
    dp_count, vp_count = mesh.shape["dp"], mesh.shape["vp"]

    def local_step(hidden, targets, loss_mask, norm_scale, w_head):
        vocab = w_head.shape[1]
        dp, vp = lax.axis_index("dp"), lax.axis_index("vp")
        g = norm_scale.reshape(1, DIM)

        mask = loss_mask[0]
        idx = lax.iota(i32, BLK)
        before = jnp.sum(jnp.where(idx[None, :] < idx[:, None], mask[None, :], 0), axis=1)
        kept = jnp.sum(mask)
        pos = jnp.where(mask == 1, before, kept + idx - before)
        perm = pos[None, :] == idx[:, None]
        x_sorted = jnp.dot(perm.astype(bf16), hidden[0], preferred_element_type=f32)
        t_sorted = jnp.sum(jnp.where(perm, targets[0][None, :], 0), axis=1)
        inv_rms = lax.rsqrt(jnp.mean(x_sorted * x_sorted, axis=-1, keepdims=True) + EPS)
        x_hat = x_sorted * inv_rms

        core_pairs = [(v, v ^ 1) for v in range(vp_count)]
        x_pairs = [(v, v ^ 2) for v in range(vp_count)]
        from_core = lax.ppermute(x_hat, "vp", core_pairs)
        from_x = lax.ppermute(x_hat, "vp", x_pairs)
        xh_all = lax.all_gather(x_hat, ("dp", "vp"), axis=0, tiled=True)
        n_near, st_near = forward_stats(FWD_GROUP, x_hat, from_core, g, w_head)
        from_x_core = lax.ppermute(from_x, "vp", core_pairs)
        n_far, st_far = forward_stats(FWD_GROUP, from_x, from_x_core, g, w_head)

        info = jnp.stack([t_sorted.astype(f32), jnp.full((BLK,), kept.astype(f32))])[None]
        near = lax.all_gather(jnp.concatenate([st_near, st_far, info]), "vp", axis=0)
        stats = jnp.stack([jnp.stack([near[v, b ^ v] for b in range(vp_count)]) for v in range(vp_count)])
        row_max = jnp.max(stats[:, :, 0], axis=0)
        row_sum = jnp.sum(stats[:, :, 1] * jnp.exp(stats[:, :, 0] - row_max), axis=0)
        lse_row = row_max + jnp.log(row_sum)
        info_row = near[:, vp_count]
        lse_row = jnp.where(idx[None, :].astype(f32) < info_row[:, 1], lse_row, DROPPED)
        info_all = lax.all_gather(jnp.concatenate([lse_row[:, None], info_row], axis=1), "dp", axis=0, tiled=True)
        lse_all, t_all, kept_all = info_all[:, 0], info_all[:, 1], info_all[:, 2, 0].astype(i32)

        weight = 1.0 / jnp.sum(kept_all).astype(f32)
        live = idx[None, :] < kept_all[:, None]
        w_all = jnp.where(live, weight, 0.0)
        lse_all = jnp.where(live, lse_all * LOG2E - jnp.log2(weight), DROPPED)
        none = jnp.zeros_like(w_all)
        aux_all = jnp.stack([lse_all, w_all, t_all] + [none] * 5, axis=1)

        span = (kept_all + ALIGN - 1) // ALIGN * ALIGN
        blocks = dp_count * vp_count
        before = lax.iota(i32, blocks)[None, :] < lax.iota(i32, blocks + 1)[:, None]
        offs = jnp.sum(jnp.where(before, span[None, :], 0), axis=1)
        count = offs[blocks:]

        first = dp * vp_count
        kept_row = lax.dynamic_slice(kept_all, (first,), (vp_count,))
        span_row = lax.dynamic_slice(span, (first,), (vp_count,))
        aux_row = lax.dynamic_slice(aux_all, (first, 0, 0), (vp_count, 8, BLK))
        offs_row = lax.dynamic_slice(offs, (first,), (vp_count,)) - lax.dynamic_slice(offs, (first,), (1,))
        nt_row = ((jnp.sum(span_row) + BLK - 1) // BLK).reshape(1)
        mine = jnp.bitwise_xor(jnp.arange(vp_count, dtype=i32), vp)
        y_pairs = [(d, d ^ 1) for d in range(dp_count)]
        z_pairs = [(d, d ^ 2) for d in range(dp_count)]
        y_jobs, z_jobs, own_jobs, base = [], [], [], 0
        for widths, jobs, pairs in ((Y_WIDTHS, y_jobs, y_pairs), (Z_WIDTHS, z_jobs, z_pairs), (OWN_WIDTHS, own_jobs, None)):
            for n in dict.fromkeys(widths):
                stride = n * widths.count(n)
                jobs += [
                    (n, base + n * c, stride if pairs is y_pairs else 0, stride if pairs is z_pairs else 0, pairs)
                    for c in range(widths.count(n))
                ]
                base += stride * (2 if pairs else 1)
        jobs = [job for pair in zip(y_jobs, z_jobs) for job in pair] + own_jobs
        start, y_step, z_step, v_step = (
            jnp.array([x for job in jobs for x in entries(job)], i32)
            for entries in (
                lambda j: (j[1] // j[0], j[1], j[1], j[1] + j[2] + j[3]),
                lambda j: (j[2] // j[0], j[2], j[2], -j[2]),
                lambda j: (j[3] // j[0], j[3], j[3], -j[3]),
                lambda j: (0, vocab, 0, 0),
            )
        )
        table = start + y_step * (dp % 2) + z_step * (dp // 2 % 2) + v_step * vp
        aux_row, offs, count, table, aux_all = lax.optimization_barrier((aux_row, offs, count, table, aux_all))

        dn_part, t_part = backward_dn(
            offs_row, span_row, kept_row, mine, nt_row, (vp * vocab).reshape(1), n_near, n_far, aux_row, w_head
        )
        d_normed = lax.psum_scatter(dn_part, "vp", scatter_dimension=0, tiled=True)

        d_scale = jnp.sum(d_normed * x_hat, axis=0)
        e = d_normed * norm_scale
        d_x = inv_rms * (e - x_hat * jnp.mean(e * x_hat, axis=-1, keepdims=True))
        back = perm.astype(bf16).T
        d_x = jnp.dot(back, d_x.astype(bf16), preferred_element_type=f32).astype(bf16)
        lse_own = lax.dynamic_slice(lse_row, (vp, 0), (1, BLK))[0]
        loss_part = weight * jnp.sum(jnp.where(idx < kept, lse_own, 0.0)) - jnp.sum(t_part)
        parts = jnp.concatenate([d_scale.reshape(6, 128), jnp.full((58, 128), loss_part, f32)])
        parts = lax.all_gather(parts, ("dp", "vp"), axis=0)
        parts = jnp.sum(parts[:, :8], axis=0)

        n_all, auxc_all, chunk = first_columns(offs, table, xh_all, aux_all, g, w_head)
        own, whole, moved = (chunk, 2), None, []
        for k, (width, *_, pairs) in enumerate(jobs):
            if k:
                merges = [own] if k == 1 else [moved[k - LAG]] if k >= LAG else []
                chunk, whole = weight_grad(k, width, table, count, n_all, auxc_all, w_head, whole, merges)
            if pairs:
                moved.append((lax.ppermute(chunk, "dp", pairs), 4 * k + 3))
        whole = finish(table, whole, moved[len(jobs) - LAG :])
        return parts[6, 0], d_x[None], whole, parts[:6].reshape(DIM)

    return jax.shard_map(
        local_step,
        mesh=mesh,
        in_specs=(P("dp", "vp", None), P("dp", "vp"), P("dp", "vp"), P(None), P(None, "vp")),
        out_specs=(P(), P("dp", "vp", None), P(None, "vp"), P(None)),
        check_vma=False,
    )
```
